32 devices in a mesh: row: 4 (over y, core), col: 8 (over z, x).
Axes of the slice: x: 2, y: 2, z: 4, core: 2. Of those that a mesh axis runs over, the one named last changes fastest.
Arguments:
- points: float32 [1280, 128], P(('row', 'col')), may hold values from -6 to 6
- source_ids: int32 [1280], P(('row', 'col')), may hold values from 0 to 63
- source_shift: float32 [64, 128], replicated, may hold values from -4 to 4
- noise_level: float32 [64], replicated, may hold values from 0.1 to 1
- weight_in: float32 [128, 256], replicated, may hold values from -0.5 to 0.5
- bias_in: float32 [256], replicated, may hold values from -3 to 3
- weight_out: float32 [256, 32], replicated, may hold values from -0.375 to 0.375
- inverse_scale: float32 [32], replicated, may hold values from 0.15 to 0.6
- frequency: float32 [32, 256], replicated, may hold values from -5 to 5
- phase_shift: float32 [256], replicated, may hold values from -3.140625 to 3.140625
- solution: float32 [1280, 128], P(('row', 'col')), may hold values from -6 to 6
- residual: float32 [1280, 128], P(('row', 'col')), may hold values from -6 to 6
- direction: float32 [1280, 128], P(('row', 'col')), may hold values from -6 to 6
- prior_product: float32 [128], replicated, may hold values from 80 to 640
Outputs:
- new_solution: float32 [1280, 128], P(('row', 'col'))
- new_residual: float32 [1280, 128], P(('row', 'col'))
- new_direction: float32 [1280, 128], P(('row', 'col'))
- new_product: float32 [128], replicated
The draws below stay inside these ranges and needn't reach their ends.
All inputs are finite; a program needn't handle non-finite values.
Results may differ from the reference program's by a relative error of at most 0.00024.
Values sent between devices are 32-bit elements; how exact they have to be, the bound alone decides.
A program may use at most 64 MiB of HBM per device.

```python
import math
import jax
import jax.numpy as jnp
from jax import lax

IN_DIM = 128
HIDDEN_SIZE = 256
FEAT = 32
RHS = 128
RANK = 256
SOURCES = 64
TOTAL = 1280


def plant(drawn, own_key, smallest, largest):
    dims = drawn.shape
    index_at = [jax.random.randint(jax.random.fold_in(own_key, axis), (), 0, dims[axis]) for axis in range(len(dims))]
    drawn = drawn.at[tuple(index_at)].set(smallest)
    longest = dims.index(max(dims))
    index_at[longest] = (index_at[longest] + 1) % dims[longest]
    return drawn.at[tuple(index_at)].set(largest)


def block_scale(rng, shape, split, low, high):
    gain = 1.0
    for dim, blocks in split:
        heights = jax.random.uniform(jax.random.fold_in(jax.random.fold_in(rng, 6), dim), (blocks,), jnp.float32, low / len(split), high / len(split))
        gain = gain * jnp.repeat(jnp.exp(heights), shape[dim] // blocks).reshape((-1,) + (1,) * (len(shape) - 1 - dim))
    return gain


def normal_values(stream_key, dims, scale, reach, cuts=(), kind=jnp.bfloat16):
    result = jax.random.normal(stream_key, dims, jnp.float32) * scale
    if len(cuts) > 0:
        result = block_scale(stream_key, dims, cuts, -0.22, 0.18) * result
    return jnp.clip(result, min=-reach, max=reach).astype(kind)


def setup_inputs(seed: int = 0) -> dict:
    seeds = jax.random.split(jax.random.key(seed), 15)
    points = normal_values(seeds[0], (TOTAL, IN_DIM), 1.0, 6.0, ((0, 32),), jnp.float32)
    source_ids = plant(jax.random.randint(seeds[1], (TOTAL,), 0, SOURCES), jax.random.fold_in(seeds[1], 1), 0, SOURCES - 1).astype(jnp.int32)
    source_shift = normal_values(seeds[2], (SOURCES, IN_DIM), 0.7, 4.0, (), jnp.float32)
    noise_level = jnp.clip(jnp.exp(jax.random.uniform(seeds[3], (SOURCES,), jnp.float32, math.log(0.1), math.log(1.0))), 0.1, 1.0)
    weight_in = normal_values(seeds[4], (IN_DIM, HIDDEN_SIZE), IN_DIM ** -0.5, 0.5, (), jnp.float32)
    bias_in = normal_values(seeds[5], (HIDDEN_SIZE,), 0.7, 3.0, (), jnp.float32)
    weight_out = normal_values(seeds[6], (HIDDEN_SIZE, FEAT), HIDDEN_SIZE ** -0.5, 0.375, (), jnp.float32)
    inverse_scale = jnp.clip(jnp.exp(jax.random.uniform(seeds[7], (FEAT,), jnp.float32, math.log(0.15), math.log(0.6))), 0.15, 0.6)
    frequency = normal_values(seeds[8], (FEAT, RANK), 1.0, 5.0, (), jnp.float32)
    phase_shift = jnp.clip(jax.random.uniform(seeds[9], (RANK,), jnp.float32, -3.140625, 3.140625), -3.140625, 3.140625)
    solution = normal_values(seeds[10], (TOTAL, RHS), 1.0, 6.0, ((0, 32),), jnp.float32)
    residual = normal_values(seeds[11], (TOTAL, RHS), 1.0, 6.0, ((0, 32),), jnp.float32)
    direction = normal_values(seeds[12], (TOTAL, RHS), 1.0, 6.0, ((0, 32),), jnp.float32)
    prior_product = jnp.clip(jnp.exp(jax.random.uniform(seeds[13], (RHS,), jnp.float32, math.log(80.0), math.log(640.0))), 80.0, 640.0)
    return dict(points=points, source_ids=source_ids, source_shift=source_shift, noise_level=noise_level, weight_in=weight_in, bias_in=bias_in, weight_out=weight_out, inverse_scale=inverse_scale, frequency=frequency, phase_shift=phase_shift, solution=solution, residual=residual, direction=direction, prior_product=prior_product)


HIGH = lax.Precision.HIGHEST

def reference(points, source_ids, source_shift, noise_level, weight_in, bias_in, weight_out, inverse_scale, frequency, phase_shift, solution, residual, direction, prior_product):
    onehot = (source_ids[:, None] == jnp.arange(source_shift.shape[0], dtype=jnp.int32)[None, :]).astype(jnp.float32)
    shifted = points + jnp.dot(onehot, source_shift, precision=HIGH)
    hidden = jnp.tanh(jnp.dot(shifted, weight_in, precision=HIGH) + bias_in)
    scaled = jnp.dot(hidden, weight_out, precision=HIGH) * inverse_scale
    noise = jnp.dot(onehot, noise_level, precision=HIGH)
    squares = lax.optimization_barrier(jnp.sum(scaled * scaled, axis=1))
    total = scaled.shape[0]
    block_rows = math.gcd(total, 1024)
    blocks = scaled.reshape(total // block_rows, block_rows, scaled.shape[1])

    def apply_block(rows_feat):
        row_sq = lax.optimization_barrier(jnp.sum(rows_feat * rows_feat, axis=1))
        distance = row_sq[:, None] + squares[None, :] - 2.0 * jnp.dot(rows_feat, scaled.T, precision=HIGH)
        return jnp.dot(jnp.exp(-0.5 * distance), direction, precision=HIGH)
    kernel_part = lax.map(apply_block, blocks).reshape(total, direction.shape[1])
    image = kernel_part + noise[:, None] * direction
    curvature = lax.optimization_barrier(jnp.sum(direction * image, axis=0))
    alpha = prior_product / curvature
    new_solution = solution + alpha * direction
    new_residual = residual - alpha * image
    rank = frequency.shape[1]
    basis = jnp.sqrt(2.0 / rank) * jnp.cos(jnp.dot(scaled, frequency, precision=HIGH) + phase_shift)
    capacity = jnp.eye(rank, dtype=jnp.float32) + jnp.dot(basis.T, basis / noise[:, None], precision=HIGH)
    projected = jnp.dot(basis.T, new_residual / noise[:, None], precision=HIGH)
    lower = jnp.linalg.cholesky(capacity)
    middle = lax.linalg.triangular_solve(lower, projected, left_side=True, lower=True)
    coeffs = lax.linalg.triangular_solve(lower, middle, left_side=True, lower=True, transpose_a=True)
    precond = (new_residual - jnp.dot(basis, coeffs, precision=HIGH)) / noise[:, None]
    new_product = lax.optimization_barrier(jnp.sum(new_residual * precond, axis=0))
    new_direction = precond + new_product / prior_product * direction
    return (new_solution, new_residual, new_direction, new_product)
```

```python
import functools
import math

import jax
import jax.numpy as jnp
from jax import lax
from jax.experimental import pallas as pl
from jax.experimental.pallas import tpu as pltpu
from jax.sharding import PartitionSpec as P
HIGH = lax.Precision.HIGHEST
MESH = pl.DeviceIdType.MESH
VMEM = pl.BlockSpec(memory_space=pltpu.VMEM)


def mm(a, b, ca=1, cb=0):
    return lax.dot_general(
        a, b, (((ca,), (cb,)), ((), ())), precision=HIGH, preferred_element_type=jnp.float32
    )


def cosine(x):
    n = jnp.floor(x * 0.3183098861837907 + 0.5)
    r = ((x - n * 3.140625) - n * 9.67502593994140625e-4) - n * 1.509957990978376432e-7
    half = n * 0.5
    sign = 1.0 - 4.0 * (half - jnp.floor(half))
    z = r * r
    p = 2.08767569878681e-9
    for c in (
        -2.75573192239859e-7,
        2.48015873015873e-5,
        -1.38888888888889e-3,
        4.16666666666667e-2,
        -0.5,
        1.0,
    ):
        p = p * z + c
    return sign * p


def invert_block(m):
    size = m.shape[0]
    m = m.reshape(size // 8, 8, size)
    shape = m.shape
    lane = lax.broadcasted_iota(jnp.int32, (8, size), 1)
    sub = lax.broadcasted_iota(jnp.int32, (8, size), 0)
    for k in range(0, size, 4):
        group, off = divmod(k, 8)
        cols = [jnp.broadcast_to(m[:, :, k + j : k + j + 1], shape) for j in range(4)]
        own = m[group]
        rows = [jnp.broadcast_to(own[off + i : off + i + 1, :], (8, size)) for i in range(4)]

        def at(i, j):
            return jnp.broadcast_to(cols[j][group][off + i : off + i + 1, :], (8, size))

        a00, a01, a11 = at(0, 0), at(0, 1), at(1, 1)
        b00, b01, b10, b11 = at(0, 2), at(0, 3), at(1, 2), at(1, 3)
        d00, d01, d11 = at(2, 2), at(2, 3), at(3, 3)
        inv = 1.0 / (a00 * a11 - a01 * a01)
        e00, e01, e11 = a11 * inv, -a01 * inv, a00 * inv
        f00, f01 = e00 * b00 + e01 * b10, e00 * b01 + e01 * b11
        f10, f11 = e01 * b00 + e11 * b10, e01 * b01 + e11 * b11
        s00 = d00 - (b00 * f00 + b10 * f10)
        s01 = d01 - (b00 * f01 + b10 * f11)
        s11 = d11 - (b01 * f01 + b11 * f11)
        inv = 1.0 / (s00 * s11 - s01 * s01)
        t00, t01, t11 = s11 * inv, -s01 * inv, s00 * inv
        g00, g01 = f00 * t00 + f01 * t01, f00 * t01 + f01 * t11
        g10, g11 = f10 * t00 + f11 * t01, f10 * t01 + f11 * t11
        p00 = e00 + g00 * f00 + g01 * f01
        p01 = e01 + g00 * f10 + g01 * f11
        p11 = e11 + g10 * f10 + g11 * f11
        pivots = (
            (p00, p01, -g00, -g01),
            (p01, p11, -g10, -g11),
            (-g00, -g10, t00, t01),
            (-g01, -g11, t01, t11),
        )
        masks = [lane == k + j for j in range(4)]
        inside = (lane >= k) & (lane < k + 4)
        rows = [
            jnp.where(masks[j], 1.0, jnp.where(inside, 0.0, rows[j])) for j in range(4)
        ]
        scaled = [
            (pivots[i][0] * rows[0] + pivots[i][1] * rows[1])
            + (pivots[i][2] * rows[2] + pivots[i][3] * rows[3])
            for i in range(4)
        ]
        base = jnp.where(inside[None], 0.0, m)
        update = (cols[0] * scaled[0][None] + cols[1] * scaled[1][None]) + (
            cols[2] * scaled[2][None] + cols[3] * scaled[3][None]
        )
        m = base - update
        fixed = m[group]
        for i in range(4):
            fixed = jnp.where(sub == off + i, scaled[i], fixed)
        pieces = [fixed[None]]
        if group > 0:
            pieces.insert(0, m[:group])
        if group + 1 < size // 8:
            pieces.append(m[group + 1 :])
        m = jnp.concatenate(pieces, axis=0) if len(pieces) > 1 else pieces[0]
    return m.reshape(size, size)


def invert(a):
    size = a.shape[0]
    if size <= 128:
        return invert_block(a)
    h = size // 2
    top, cross, low = a[:h, :h], a[:h, h:], a[h:, h:]
    x = invert(top)
    y = mm(x, cross)
    z = invert(low - mm(cross, y, 0, 0))
    yz = mm(y, z)
    first = jnp.concatenate([x + mm(yz, y, 1, 1), -yz], axis=1)
    second = jnp.concatenate([-yz.T, z], axis=1)
    return jnp.concatenate([first, second], axis=0)


class Peers:
    def __init__(self, rows, cols):
        self.cols, self.count = cols, rows * cols
        self.me = lax.axis_index("row") * cols + lax.axis_index("col")

    def id(self, d):
        t = lax.rem(self.me + d, self.count)
        return t, {"row": t // self.cols, "col": lax.rem(t, self.cols)}

    def each(self, body):
        def turn(d, carry):
            body(*self.id(d))
            return carry

        lax.fori_loop(1, self.count, turn, 0)

    def greet(self):
        barrier = pltpu.get_barrier_semaphore()
        self.each(
            lambda t, dev: pl.semaphore_signal(barrier, inc=1, device_id=dev, device_id_type=MESH)
        )

    def meet(self):
        pl.semaphore_wait(pltpu.get_barrier_semaphore(), self.count - 1)

    def send(self, src, dst, send_sem, recv_sem, dev):
        pltpu.make_async_remote_copy(
            src_ref=src,
            dst_ref=dst,
            send_sem=send_sem,
            recv_sem=recv_sem,
            device_id=dev,
            device_id_type=MESH,
        ).start()


def take(ref, sem):
    pltpu.make_async_copy(ref, ref, sem).wait()


def features(points, ids, shift, level, w_in, b_in, w_out, inv_scale):
    n = points.shape[0]
    sources = shift.shape[0]
    onehot = (lax.broadcasted_iota(jnp.int32, (sources, n), 0) == ids).astype(jnp.float32)
    eye = lax.broadcasted_iota(jnp.int32, (sources, sources), 0) == lax.broadcasted_iota(
        jnp.int32, (sources, sources), 1
    )
    diag = jnp.where(eye, level, 0.0)
    spread = mm(diag, jnp.ones((sources, 128), jnp.float32))
    noise = mm(onehot, spread, 0, 0)
    shifted = points + mm(onehot, shift, 0, 0)
    hidden = jnp.tanh(mm(shifted, w_in) + b_in)
    scaled = mm(hidden, w_out, 1, 1) * inv_scale
    return scaled, noise


def layout(n, feat):
    groups, per = n // 8, 128 // feat
    return groups, per, -(-(groups + 1) // per)


def pack(scaled, noise):
    n, feat = scaled.shape
    groups, per, tiles = layout(n, feat)
    lane = lax.broadcasted_iota(jnp.int32, (8, feat), 1)
    levels = jnp.zeros((8, feat), jnp.float32)
    for g in range(groups):
        levels = jnp.where(lane == g, noise[8 * g : 8 * g + 8, :feat], levels)
    pieces = [scaled[8 * g : 8 * g + 8] for g in range(groups)] + [levels]
    pieces += [jnp.zeros((8, feat), jnp.float32)] * (per * tiles - groups - 1)
    return jnp.concatenate(
        [jnp.concatenate(pieces[per * t : per * (t + 1)], axis=1) for t in range(tiles)], axis=0
    )


def unpack(packed, n, feat):
    groups, per, tiles = layout(n, feat)
    pieces = []
    for first in range(0, packed.shape[0], 8 * tiles):
        for g in range(groups):
            at, lane = first + 8 * (g // per), feat * (g % per)
            pieces.append(packed[at : at + 8, lane : lane + feat])
    return jnp.concatenate(pieces, axis=0)


def gather_kernel(
    dims, points, ids, shift, level, w_in, b_in, w_out, inv_scale, direction,
    feat_all, dir_col, own, row_feat, col_feat, send_sem, recv_sem,
):
    peers = Peers(*dims)
    rows, cols = dims
    n, feat = points.shape[0], w_out.shape[0]
    high = 8 * layout(n, feat)[2]
    r, c = lax.axis_index("row"), lax.axis_index("col")
    peers.greet()
    scaled, noise = features(
        points[...], ids[...], shift[...], level[...], w_in[...], b_in[...], w_out[...], inv_scale[...]
    )
    mine = pl.ds(pl.multiple_of(peers.me * high, 8), high)
    feat_all[mine, :] = pack(scaled, noise)
    own[...] = jnp.concatenate([scaled, noise[:, feat:]], axis=1)
    block = pl.ds(pl.multiple_of(r * n, 8), n)
    dir_col[block, :] = direction[...]
    peers.meet()
    peers.each(
        lambda t, dev: peers.send(
            feat_all.at[mine], feat_all.at[mine], send_sem.at[0], recv_sem.at[0], dev
        )
    )

    def turn(d, carry):
        dev = {"row": lax.rem(r + d, rows), "col": c}
        peers.send(direction, dir_col.at[block], send_sem.at[1], recv_sem.at[1], dev)
        return carry

    lax.fori_loop(1, rows, turn, 0)
    others = pl.ds(0, (peers.count - 1) * high)
    other_rows = pl.ds(0, (rows - 1) * n)
    take(feat_all.at[others], recv_sem.at[0])
    row_feat[...] = feat_all[pl.ds(pl.multiple_of(r * (cols * high), 8), cols * high), :]
    for q in range(rows):
        col_feat[q * high : (q + 1) * high, :] = feat_all[
            pl.ds(pl.multiple_of((q * cols + c) * high, 8), high), :
        ]
    take(dir_col.at[other_rows], recv_sem.at[1])
    take(feat_all.at[others], send_sem.at[0])
    take(dir_col.at[other_rows], send_sem.at[1])


def local_kernel(
    n, feat_all, dir_col, row_feat, col_feat, own, freq, phase, inverse, capacity, partial, basis_own
):
    feat, rank = freq.shape
    groups, per, tiles = layout(n, feat)
    amp = math.sqrt(2.0 / rank)
    count = feat_all.shape[0] // (8 * tiles)
    diag = lax.broadcasted_iota(jnp.int32, (rank, rank), 0) == lax.broadcasted_iota(
        jnp.int32, (rank, rank), 1
    )
    capacity[...] = jnp.where(diag, 1.0, 0.0)
    view = feat_all[...].reshape(count, tiles, 8, 128)
    levels = view[:, groups // per].reshape(count * 8, 128)
    first = feat * (groups % per)
    for g in range(groups):
        block = view[:, g // per].reshape(count * 8, 128)
        above, below = feat * (g % per), 128 - feat * (g % per + 1)
        wide = [freq[...]]
        if above:
            wide.insert(0, jnp.zeros((above, rank), jnp.float32))
        if below:
            wide.append(jnp.zeros((below, rank), jnp.float32))
        basis = amp * cosine(mm(block, jnp.concatenate(wide, axis=0)) + phase[...])
        capacity[...] += mm(basis, basis / levels[:, first + g : first + g + 1], 0, 0)
    basis_own[...] = amp * cosine(mm(own[...][:, :feat], freq[...]) + phase[...])
    over = unpack(row_feat[...], n, feat)
    under = unpack(col_feat[...], n, feat)
    sq_over = jnp.sum(over * over, axis=1, keepdims=True)
    sq_under = mm(jnp.ones((8, feat), jnp.float32), under * under, 1, 1)[0:1, :]
    distance = sq_over + sq_under - 2.0 * mm(over, under, 1, 1)
    partial[...] = mm(jnp.exp(-0.5 * distance), dir_col[...])
    inverse[...] = invert(capacity[...])


def reduce_kernel(
    dims, owners, own, partial, direction, residual, basis, prior,
    sums, projected, image,
    sums_all, part, slots, blocks, send_sem, recv_sem,
):
    peers = Peers(*dims)
    me, count = peers.me, peers.count
    cols = dims[1]
    n, rhs = direction.shape
    r, c = lax.axis_index("row"), lax.axis_index("col")
    peers.greet()
    noise = own[...][:, 127:128]
    res, d = residual[...], direction[...]
    sres = res / noise
    block = pl.ds(pl.multiple_of(c * n, 8), n)
    blocks[block, :] = partial[block, :]
    peers.meet()

    def turn(k, carry):
        t = lax.rem(c + k, cols)
        peers.send(
            partial.at[pl.ds(pl.multiple_of(t * n, 8), n)],
            blocks.at[block], send_sem.at[3], recv_sem.at[3], {"row": r, "col": t},
        )
        return carry

    lax.fori_loop(1, cols, turn, 0)
    rank = projected.shape[0]
    rq = rank // owners
    proj_res = mm(basis[...], sres, 0, 0).reshape(owners, 1, rq, rhs)
    other_cols = pl.ds(0, (cols - 1) * n)
    take(blocks.at[other_cols], recv_sem.at[3])
    img = jnp.sum(blocks[...].reshape(cols, n, rhs), axis=0) + noise * d
    image[...] = img
    simg = img / noise
    mine = pl.ds(pl.multiple_of(me * 8, 8), 8)
    sums_all[mine, :] = jnp.concatenate(
        [
            jnp.sum(d * img, axis=0, keepdims=True),
            jnp.sum(res * sres, axis=0, keepdims=True),
            jnp.sum(res * simg, axis=0, keepdims=True),
            jnp.sum(img * simg, axis=0, keepdims=True),
            jnp.zeros((4, rhs), jnp.float32),
        ],
        axis=0,
    )
    proj_img = mm(basis[...], simg, 0, 0).reshape(owners, 1, rq, rhs)
    part[...] = jnp.concatenate([proj_res, proj_img], axis=1).reshape(2 * rank, rhs)
    slot = pl.ds(pl.multiple_of(me * (2 * rq), 8), 2 * rq)

    def scatter(t, dev):
        def go():
            peers.send(
                part.at[pl.ds(pl.multiple_of(t * (2 * rq), 8), 2 * rq)],
                slots.at[slot], send_sem.at[1], recv_sem.at[1], dev,
            )

        peers.send(sums_all.at[mine], sums_all.at[mine], send_sem.at[0], recv_sem.at[0], dev)
        if owners < count:
            pl.when(t < owners)(go)
        else:
            go()

    peers.each(scatter)
    other_sums = pl.ds(0, (count - 1) * 8)
    take(sums_all.at[other_sums], recv_sem.at[0])
    totals = jnp.sum(sums_all[...].reshape(count, 8, rhs), axis=0)
    sums[...] = totals
    alpha = prior[...] / totals[0:1, :]

    def owner():
        result = pl.ds(pl.multiple_of(me * rq, 8), rq)
        slots[slot, :] = part[slot, :]
        take(slots.at[pl.ds(0, (count - 1) * 2 * rq)], recv_sem.at[1])
        both = jnp.sum(slots[...].reshape(count, 2 * rq, rhs), axis=0)
        projected[result, :] = both[:rq] - alpha * both[rq:]
        if owners > 1:
            take(part.at[pl.ds(0, (owners - 1) * 2 * rq)], send_sem.at[1])
        peers.each(
            lambda t, dev: peers.send(
                projected.at[result], projected.at[result], send_sem.at[2], recv_sem.at[2], dev
            )
        )
        if owners > 1:
            take(projected.at[pl.ds(0, (owners - 1) * rq)], recv_sem.at[2])
        take(slots.at[pl.ds(0, (count - 1) * rq)], send_sem.at[2])

    def guest():
        take(projected, recv_sem.at[2])
        take(part, send_sem.at[1])

    if owners < count:
        pl.when(me < owners)(owner)
        pl.when(me >= owners)(guest)
    else:
        owner()
    take(sums_all.at[other_sums], send_sem.at[0])
    take(blocks.at[other_cols], send_sem.at[3])


def final_kernel(
    inverse, capacity, projected, sums, own, image, direction, residual, sol, basis, prior,
    new_sol, new_res, new_dir, new_prod,
):
    proj, tot = projected[...], sums[...]
    alpha = prior[...] / tot[0:1, :]
    coeffs = mm(inverse[...], proj)
    coeffs = coeffs + mm(inverse[...], proj - mm(capacity[...], coeffs))
    noise = own[...][:, 127:128]
    d = direction[...]
    nres = residual[...] - alpha * image[...]
    norm = tot[1:2, :] - 2.0 * alpha * tot[2:3, :] + alpha * alpha * tot[3:4, :]
    prod = norm - jnp.sum(proj * coeffs, axis=0, keepdims=True)
    precond = (nres - mm(basis[...], coeffs)) / noise
    new_sol[...] = sol[...] + alpha * d
    new_res[...] = nres
    new_dir[...] = precond + prod / prior[...] * d
    new_prod[...] = prod


def per_device(
    dims, points, source_ids, source_shift, noise_level, weight_in, bias_in, weight_out,
    inverse_scale, frequency, phase_shift, solution, residual, direction, prior_product,
):
    count = dims[0] * dims[1]
    n, rhs = direction.shape
    feat, rank = frequency.shape
    f32 = jnp.float32
    sds = jax.ShapeDtypeStruct
    row = lambda v: v.reshape(1, -1)
    dma = pltpu.SemaphoreType.DMA
    prior = row(prior_product)
    high = 8 * layout(n, feat)[2]
    feat_all, dir_col, own, row_feat, col_feat = pl.pallas_call(
        functools.partial(gather_kernel, dims),
        out_shape=(
            sds((count * high, 128), f32), sds((dims[0] * n, rhs), f32), sds((n, 128), f32),
            sds((dims[1] * high, 128), f32), sds((dims[0] * high, 128), f32),
        ),
        in_specs=[VMEM] * 9,
        out_specs=(VMEM,) * 5,
        scratch_shapes=[dma((2,)), dma((2,))],
        compiler_params=pltpu.CompilerParams(collective_id=0, has_side_effects=True),
        name="gather",
    )(
        points, row(source_ids), source_shift, row(noise_level), weight_in, row(bias_in),
        weight_out.T, row(inverse_scale), direction,
    )
    phase = row(phase_shift)
    square = sds((rank, rank), f32)
    inverse, capacity, partial, basis = pl.pallas_call(
        functools.partial(local_kernel, n),
        out_shape=(square, square, sds((dims[1] * n, rhs), f32), sds((n, rank), f32)),
        in_specs=[VMEM] * 7,
        out_specs=(VMEM,) * 4,
        name="local",
    )(feat_all, dir_col, row_feat, col_feat, own, frequency, phase)
    owners = min(count, rank // 8)
    sums, projected, image = pl.pallas_call(
        functools.partial(reduce_kernel, dims, owners),
        out_shape=(sds((8, rhs), f32), sds((rank, rhs), f32), sds((n, rhs), f32)),
        in_specs=[VMEM] * 6,
        out_specs=(VMEM,) * 3,
        scratch_shapes=[
            pltpu.VMEM((8 * count, rhs), f32),
            pltpu.VMEM((2 * rank, rhs), f32),
            pltpu.VMEM((count * (2 * rank // owners), rhs), f32),
            pltpu.VMEM((dims[1] * n, rhs), f32),
            dma((4,)),
            dma((4,)),
        ],
        compiler_params=pltpu.CompilerParams(collective_id=1, has_side_effects=True),
        name="reduce",
    )(own, partial, direction, residual, basis, prior)
    block = sds((n, rhs), f32)
    new_sol, new_res, new_dir, new_prod = pl.pallas_call(
        final_kernel,
        out_shape=(block, block, block, sds((1, rhs), f32)),
        in_specs=[VMEM] * 11,
        out_specs=(VMEM,) * 4,
        name="final",
    )(inverse, capacity, projected, sums, own, image, direction, residual, solution, basis, prior)
    return new_sol, new_res, new_dir, new_prod.reshape(rhs)


BF16 = jnp.bfloat16


def dot(a, b, ca=1, cb=0):
    return lax.dot_general(a, b, (((ca,), (cb,)), ((), ())), preferred_element_type=jnp.float32)


def split(x):
    high = x.astype(BF16)
    rest = x - high.astype(jnp.float32)
    mid = rest.astype(BF16)
    low = (rest - mid.astype(jnp.float32)).astype(BF16)
    return high, mid, low


def rows_of(x):
    parts = [p.astype(jnp.float32) for p in split(x)]
    fill = -3 * x.shape[0] % 16
    if fill:
        parts.append(jnp.zeros((fill, x.shape[1]), jnp.float32))
    return jnp.concatenate(parts, axis=0).astype(BF16)


def fold(acc, q):
    return acc[0:q] + acc[q : 2 * q] + acc[2 * q : 3 * q]


def iota(shape, dim):
    return lax.broadcasted_iota(jnp.int32, shape, dim)


class Plan:
    def __init__(self, dims, n, rhs, feat):
        self.count = dims[0] * dims[1]
        self.n, self.rhs, self.feat = n, rhs, feat
        self.q = rhs // self.count
        self.per = 128 // n
        self.windows = -(-self.count // self.per)
        self.wide = 128 * self.windows
        self.groups = n // 8
        self.pieces = 128 // feat - 1
        self.tiles = -(-self.groups // self.pieces)

    def fits(self):
        return (
            self.rhs == 128
            and self.rhs % self.count == 0
            and self.q % 4 == 0
            and 2 * self.n + 2 <= 128
            and self.n % 8 == 0
            and self.groups <= 8
            and self.feat % 16 == 0
            and self.feat <= 32
            and self.wide <= 2048
        )


def cosine_turns(u):
    r = u - jnp.round(u)
    z = r * r
    p = SIN[-1]
    for c in SIN[-2::-1]:
        p = p * z + c
    s = p * r
    return 1.0 - 2.0 * (s * s)


SIN = tuple((-1.0) ** i * math.pi ** (2 * i + 1) / math.factorial(2 * i + 1) for i in range(8))


def pack_tiles(plan, scaled, noise):
    feat = plan.feat
    lane = iota((8, feat), 1)
    levels = jnp.zeros((8, feat), jnp.float32)
    for g in range(plan.groups):
        levels = jnp.where(lane == g, noise[8 * g : 8 * g + 8, :feat], levels)
    tiles = []
    for t in range(plan.tiles):
        row = []
        for j in range(plan.pieces):
            g = t * plan.pieces + j
            row.append(
                scaled[8 * g : 8 * g + 8] if g < plan.groups else jnp.zeros((8, feat), jnp.float32)
            )
        tiles.append(jnp.concatenate(row + [levels], axis=1))
    return tiles


def unpack_tiles(plan, feat_all):
    n, feat, per = plan.n, plan.feat, plan.per
    group = lax.rem(iota((8, 128), 1), n) // 8
    place = lax.rem(group, plan.pieces)[0:1]
    zero = jnp.zeros((8, 128), jnp.float32)
    features, levels = [], []
    for w in range(plan.windows):
        rows = []
        for k in range(per):
            s = w * per + k
            for g in range(plan.groups):
                rows.append(feat_all[s, g // plan.pieces] if s < plan.count else zero)
        rows += [zero] * (16 - len(rows))
        turned = jnp.concatenate(rows, axis=0).T
        out = turned[(plan.pieces - 1) * feat : plan.pieces * feat]
        for j in range(plan.pieces - 1):
            out = jnp.where(place == j, turned[j * feat : (j + 1) * feat], out)
        features.append(out)
        base = plan.pieces * feat
        level = jnp.where(iota((8, 128), 0) == group, turned[base : base + 8], 0.0)
        levels.append(jnp.sum(level, axis=0, keepdims=True))
    return jnp.concatenate(features, axis=1), jnp.concatenate(levels, axis=1)


def live_lanes(plan):
    lane = iota((1, plan.wide), 1)
    inside = lax.rem(lane, 128)
    source = (lane // 128) * plan.per + inside // plan.n
    return (inside < plan.per * plan.n) & (source < plan.count)


def between(lane, start, n):
    first = start % 128
    last = first + n
    if last <= 128:
        return (lane >= first) & (lane < last)
    return (lane >= first) | (lane < last - 128)


def main_kernel(
    dims, points, ids, shift, level, w_in, b_in, w_out, inv_scale, freq, phase,
    residual, direction, prior,
    out_all,
    feat_all, turned, slabs, outs, right, left, capacity, inverse, basis, send_sem, recv_sem,
):
    peers = Peers(*dims)
    me, count = peers.me, peers.count
    n, rhs = direction.shape
    feat, rank = freq.shape
    plan = Plan(dims, n, rhs, feat)
    q, per, wide, windows = plan.q, plan.per, plan.wide, plan.windows
    f32 = jnp.float32
    peers.greet()
    scaled, noise = features(
        points[...], ids[...], shift[...], level[...], w_in[...], b_in[...], w_out[...], inv_scale[...]
    )
    for t, tile in enumerate(pack_tiles(plan, scaled, noise)):
        feat_all[me, t] = tile
    peers.meet()
    peers.each(
        lambda t, dev: peers.send(
            feat_all.at[me], feat_all.at[me], send_sem.at[0], recv_sem.at[0], dev
        )
    )
    stacked = jnp.concatenate(
        [direction[...], residual[...], prior[...], jnp.zeros((127 - 2 * n, rhs), f32)], axis=0
    )
    spun = pltpu.roll(stacked.T, n * lax.rem(me, per), 1)
    for t in range(count):
        turned[t] = spun[t * q : (t + 1) * q]
    slabs[me] = turned[me]
    peers.each(
        lambda t, dev: peers.send(
            turned.at[t], slabs.at[me], send_sem.at[1], recv_sem.at[1], dev
        )
    )
    turn = 1.0 / (2.0 * math.pi)
    both = jnp.concatenate([freq[...], phase[...], jnp.zeros((127 - feat, rank), f32)], axis=0) * turn
    fp = both.T
    fh, fm, fl = [p.astype(f32) for p in split(fp)]
    fills = 256 - 6 * feat - 3
    spectral = jnp.concatenate(
        [fh[:, :feat], fh[:, :feat], fh[:, :feat], fm[:, :feat], fm[:, :feat], fl[:, :feat]]
        + [p[:, feat : feat + 1] for p in (fh, fm, fl)]
        + [jnp.zeros((rank, fills), f32)],
        axis=1,
    ).astype(BF16)
    lane = iota((1, 128), 1)
    live = live_lanes(plan)

    take(feat_all.at[pl.ds(0, count - 1)], recv_sem.at[0])
    ft, levels = unpack_tiles(plan, feat_all)
    levels = jnp.where(live, levels, 1.0)
    rsn = jnp.where(live, lax.rsqrt(levels), 0.0)
    h, m, l = split(ft)
    scale2 = math.log2(math.e)
    ft2 = ft * scale2
    h2, m2, l2 = split(ft2)
    sq = -0.5 * jnp.sum(ft2 * ft, axis=0, keepdims=True)
    sqs = [p.astype(f32) for p in split(sq)]
    ones = jnp.ones((3, wide), f32)
    tail = 256 - 6 * feat
    rest = jnp.zeros((tail - 6, wide), f32)
    right[...] = jnp.concatenate(
        [h, m, l, h, m, h, jnp.concatenate([ones] + sqs + [rest], axis=0).astype(BF16)], axis=0
    )
    low = jnp.concatenate(
        [h2, h2, h2, m2, m2, l2, jnp.concatenate(sqs + [ones, rest], axis=0).astype(BF16)], axis=0
    )
    left[...] = low.T
    amp = math.sqrt(2.0 / rank)
    u = dot(spectral, right[...])
    c = cosine_turns(u) * (amp * rsn)
    ch, cm, cl = split(c)
    basis[0] = ch
    basis[1] = cm
    basis[2] = cl
    diag = iota((rank, rank), 0) == iota((rank, rank), 1)
    capacity[...] = (
        jnp.where(diag, 1.0, 0.0)
        + dot(ch, ch, 1, 1) + (dot(ch, cm, 1, 1) + dot(cm, ch, 1, 1))
        + (dot(cm, cm, 1, 1) + dot(ch, cl, 1, 1) + dot(cl, ch, 1, 1))
    )
    inverse[...] = invert(capacity[...])

    take(slabs.at[pl.ds(0, count - 1)], recv_sem.at[1])
    zero = jnp.zeros((q, 128), f32)
    dirs, ress = [], []
    for w in range(windows):
        own = [slabs[w * per + k] if w * per + k < count else zero for k in range(per)]
        d, r = zero, zero
        for k in range(per):
            d = jnp.where(between(lane, k * n, n), own[k], d)
            r = jnp.where(between(lane, (k + 1) * n, n), own[k], r)
        dirs.append(d)
        ress.append(pltpu.roll(r, 128 - n, 1))
    d = jnp.concatenate(dirs, axis=1)
    r = jnp.concatenate(ress, axis=1)
    mine = pltpu.roll(slabs[me], 128 - n * lax.rem(me, per), 1)
    own_prior = mine[:, 2 * n : 2 * n + 1]
    d3 = rows_of(d)
    acc = jnp.zeros((d3.shape[0], wide), f32)
    for w in range(windows):
        e = dot(left[w * 128 : (w + 1) * 128, :], right[...])
        k = jnp.exp2(e)
        kh = k.astype(BF16)
        kl = (k - kh.astype(f32)).astype(BF16)
        part = d3[:, w * 128 : (w + 1) * 128]
        acc = acc + (dot(part, kh) + dot(part, kl))
    img = fold(acc, q) + levels * d
    alpha = own_prior / jnp.sum(d * img, axis=1, keepdims=True)
    nres = r - alpha * img
    y = nres * rsn
    y3 = rows_of(y)
    proj = fold(
        dot(y3, basis[0], 1, 1) + dot(y3, basis[1], 1, 1) + dot(y3, basis[2], 1, 1), q
    )
    coeffs = mm(proj, inverse[...])
    coeffs = coeffs + mm(proj - mm(coeffs, capacity[...]), inverse[...])
    c3 = rows_of(coeffs)
    back = fold(dot(c3, basis[0]) + dot(c3, basis[1]) + dot(c3, basis[2]), q)
    precond = (y - back) * rsn
    prod = jnp.sum(nres * precond, axis=1, keepdims=True)
    ndir = precond + prod / own_prior * d
    for w in range(windows):
        part = nres[:, w * 128 : (w + 1) * 128]
        side = pltpu.roll(ndir[:, w * 128 : (w + 1) * 128], n, 1)
        for k in range(per):
            t = w * per + k
            if t < count:
                slab = jnp.where(lane == (k * n + 2 * n) % 128, alpha, prod)
                slab = jnp.where(between(lane, (k + 1) * n, n), side, slab)
                outs[t] = jnp.where(between(lane, k * n, n), part, slab)
    out_all[me] = outs[me]
    peers.each(
        lambda t, dev: peers.send(outs.at[t], out_all.at[me], send_sem.at[2], recv_sem.at[2], dev)
    )
    others = pl.ds(0, count - 1)
    take(out_all.at[others], recv_sem.at[2])
    take(feat_all.at[others], send_sem.at[0])
    take(slabs.at[others], send_sem.at[1])
    take(out_all.at[others], send_sem.at[2])


def finish_kernel(dims, got, direction, sol, new_sol, new_res, new_dir, new_prod):
    me = lax.axis_index("row") * dims[1] + lax.axis_index("col")
    n = direction.shape[0]
    per = 128 // n
    back = lax.rem(128 - n * lax.rem(me, per), 128)
    x = pltpu.roll(got[...], back, 1).T
    new_res[...] = x[0:n]
    new_dir[...] = x[n : 2 * n]
    new_sol[...] = sol[...] + x[2 * n : 2 * n + 1] * direction[...]
    new_prod[...] = x[2 * n + 1 : 2 * n + 2]


def per_device_columns(
    dims, points, source_ids, source_shift, noise_level, weight_in, bias_in, weight_out,
    inverse_scale, frequency, phase_shift, solution, residual, direction, prior_product,
):
    n, rhs = direction.shape
    feat, rank = frequency.shape
    plan = Plan(dims, n, rhs, feat)
    count, q, wide = plan.count, plan.q, plan.wide
    f32 = jnp.float32
    sds = jax.ShapeDtypeStruct
    row = lambda v: v.reshape(1, -1)
    dma = pltpu.SemaphoreType.DMA
    got = pl.pallas_call(
        functools.partial(main_kernel, dims),
        out_shape=sds((count, q, 128), f32),
        in_specs=[VMEM] * 13,
        out_specs=VMEM,
        scratch_shapes=[
            pltpu.VMEM((count, plan.tiles, 8, 128), f32),
            pltpu.VMEM((count, q, 128), f32),
            pltpu.VMEM((count, q, 128), f32),
            pltpu.VMEM((count, q, 128), f32),
            pltpu.VMEM((256, wide), BF16),
            pltpu.VMEM((wide, 256), BF16),
            pltpu.VMEM((rank, rank), f32),
            pltpu.VMEM((rank, rank), f32),
            pltpu.VMEM((3, rank, wide), BF16),
            dma((3,)),
            dma((3,)),
        ],
        compiler_params=pltpu.CompilerParams(collective_id=0, has_side_effects=True),
        name="columns",
    )(
        points, row(source_ids), source_shift, row(noise_level), weight_in, row(bias_in),
        weight_out.T, row(inverse_scale), frequency, row(phase_shift), residual, direction,
        row(prior_product),
    )
    block = sds((n, rhs), f32)
    new_sol, new_res, new_dir, new_prod = pl.pallas_call(
        functools.partial(finish_kernel, dims),
        out_shape=(block, block, block, sds((1, rhs), f32)),
        in_specs=[VMEM] * 3,
        out_specs=(VMEM,) * 4,
        name="finish",
    )(got.reshape(rhs, 128), direction, solution)
    return new_sol, new_res, new_dir, new_prod.reshape(rhs)


def dispatch(dims, *args):
    n, rhs = args[12].shape
    feat = args[8].shape[0]
    if Plan(dims, n, rhs, feat).fits():
        return per_device_columns(dims, *args)
    return per_device(dims, *args)


def solution(mesh):
    dims = (mesh.shape["row"], mesh.shape["col"])
    rows = P(("row", "col"), None)
    in_specs = (
        rows, P(("row", "col")), P(), P(), P(), P(), P(), P(), P(), P(), rows, rows, rows, P(),
    )
    return jax.shard_map(
        functools.partial(dispatch, dims),
        mesh=mesh,
        in_specs=in_specs,
        out_specs=(rows, rows, rows, P()),
        check_vma=False,
    )
```

```python
import functools
import math

import jax
import jax.numpy as jnp
from jax import lax
from jax.experimental import pallas as pl
from jax.experimental.pallas import tpu as pltpu
from jax.sharding import PartitionSpec as P
HIGH = lax.Precision.HIGHEST
MESH = pl.DeviceIdType.MESH
VMEM = pl.BlockSpec(memory_space=pltpu.VMEM)


def mm(a, b, ca=1, cb=0):
    return lax.dot_general(
        a, b, (((ca,), (cb,)), ((), ())), precision=HIGH, preferred_element_type=jnp.float32
    )


def cosine(x):
    n = jnp.floor(x * 0.3183098861837907 + 0.5)
    r = ((x - n * 3.140625) - n * 9.67502593994140625e-4) - n * 1.509957990978376432e-7
    half = n * 0.5
    sign = 1.0 - 4.0 * (half - jnp.floor(half))
    z = r * r
    p = 2.08767569878681e-9
    for c in (
        -2.75573192239859e-7,
        2.48015873015873e-5,
        -1.38888888888889e-3,
        4.16666666666667e-2,
        -0.5,
        1.0,
    ):
        p = p * z + c
    return sign * p


def invert_block(m):
    size = m.shape[0]
    m = m.reshape(size // 8, 8, size)
    shape = m.shape
    lane = lax.broadcasted_iota(jnp.int32, (8, size), 1)
    sub = lax.broadcasted_iota(jnp.int32, (8, size), 0)
    for k in range(0, size, 4):
        group, off = divmod(k, 8)
        cols = [jnp.broadcast_to(m[:, :, k + j : k + j + 1], shape) for j in range(4)]
        own = m[group]
        rows = [jnp.broadcast_to(own[off + i : off + i + 1, :], (8, size)) for i in range(4)]

        def at(i, j):
            return jnp.broadcast_to(cols[j][group][off + i : off + i + 1, :], (8, size))

        a00, a01, a11 = at(0, 0), at(0, 1), at(1, 1)
        b00, b01, b10, b11 = at(0, 2), at(0, 3), at(1, 2), at(1, 3)
        d00, d01, d11 = at(2, 2), at(2, 3), at(3, 3)
        inv = 1.0 / (a00 * a11 - a01 * a01)
        e00, e01, e11 = a11 * inv, -a01 * inv, a00 * inv
        f00, f01 = e00 * b00 + e01 * b10, e00 * b01 + e01 * b11
        f10, f11 = e01 * b00 + e11 * b10, e01 * b01 + e11 * b11
        s00 = d00 - (b00 * f00 + b10 * f10)
        s01 = d01 - (b00 * f01 + b10 * f11)
        s11 = d11 - (b01 * f01 + b11 * f11)
        inv = 1.0 / (s00 * s11 - s01 * s01)
        t00, t01, t11 = s11 * inv, -s01 * inv, s00 * inv
        g00, g01 = f00 * t00 + f01 * t01, f00 * t01 + f01 * t11
        g10, g11 = f10 * t00 + f11 * t01, f10 * t01 + f11 * t11
        p00 = e00 + g00 * f00 + g01 * f01
        p01 = e01 + g00 * f10 + g01 * f11
        p11 = e11 + g10 * f10 + g11 * f11
        pivots = (
            (p00, p01, -g00, -g01),
            (p01, p11, -g10, -g11),
            (-g00, -g10, t00, t01),
            (-g01, -g11, t01, t11),
        )
        masks = [lane == k + j for j in range(4)]
        inside = (lane >= k) & (lane < k + 4)
        rows = [
            jnp.where(masks[j], 1.0, jnp.where(inside, 0.0, rows[j])) for j in range(4)
        ]
        scaled = [
            (pivots[i][0] * rows[0] + pivots[i][1] * rows[1])
            + (pivots[i][2] * rows[2] + pivots[i][3] * rows[3])
            for i in range(4)
        ]
        base = jnp.where(inside[None], 0.0, m)
        update = (cols[0] * scaled[0][None] + cols[1] * scaled[1][None]) + (
            cols[2] * scaled[2][None] + cols[3] * scaled[3][None]
        )
        m = base - update
        fixed = m[group]
        for i in range(4):
            fixed = jnp.where(sub == off + i, scaled[i], fixed)
        pieces = [fixed[None]]
        if group > 0:
            pieces.insert(0, m[:group])
        if group + 1 < size // 8:
            pieces.append(m[group + 1 :])
        m = jnp.concatenate(pieces, axis=0) if len(pieces) > 1 else pieces[0]
    return m.reshape(size, size)


def invert(a):
    size = a.shape[0]
    if size <= 128:
        return invert_block(a)
    h = size // 2
    top, cross, low = a[:h, :h], a[:h, h:], a[h:, h:]
    x = invert(top)
    y = mm(x, cross)
    z = invert(low - mm(cross, y, 0, 0))
    yz = mm(y, z)
    first = jnp.concatenate([x + mm(yz, y, 1, 1), -yz], axis=1)
    second = jnp.concatenate([-yz.T, z], axis=1)
    return jnp.concatenate([first, second], axis=0)


class Peers:
    def __init__(self, rows, cols):
        self.cols, self.count = cols, rows * cols
        self.me = lax.axis_index("row") * cols + lax.axis_index("col")

    def id(self, d):
        t = lax.rem(self.me + d, self.count)
        return t, {"row": t // self.cols, "col": lax.rem(t, self.cols)}

    def each(self, body):
        def turn(d, carry):
            body(*self.id(d))
            return carry

        lax.fori_loop(1, self.count, turn, 0)

    def greet(self):
        barrier = pltpu.get_barrier_semaphore()
        self.each(
            lambda t, dev: pl.semaphore_signal(barrier, inc=1, device_id=dev, device_id_type=MESH)
        )

    def meet(self):
        pl.semaphore_wait(pltpu.get_barrier_semaphore(), self.count - 1)

    def send(self, src, dst, send_sem, recv_sem, dev):
        pltpu.make_async_remote_copy(
            src_ref=src,
            dst_ref=dst,
            send_sem=send_sem,
            recv_sem=recv_sem,
            device_id=dev,
            device_id_type=MESH,
        ).start()


def take(ref, sem):
    pltpu.make_async_copy(ref, ref, sem).wait()


def features(points, ids, shift, level, w_in, b_in, w_out, inv_scale):
    n = points.shape[0]
    sources = shift.shape[0]
    onehot = (lax.broadcasted_iota(jnp.int32, (sources, n), 0) == ids).astype(jnp.float32)
    eye = lax.broadcasted_iota(jnp.int32, (sources, sources), 0) == lax.broadcasted_iota(
        jnp.int32, (sources, sources), 1
    )
    diag = jnp.where(eye, level, 0.0)
    spread = mm(diag, jnp.ones((sources, 128), jnp.float32))
    noise = mm(onehot, spread, 0, 0)
    shifted = points + mm(onehot, shift, 0, 0)
    hidden = jnp.tanh(mm(shifted, w_in) + b_in)
    scaled = mm(hidden, w_out, 1, 1) * inv_scale
    return scaled, noise


def layout(n, feat):
    groups, per = n // 8, 128 // feat
    return groups, per, -(-(groups + 1) // per)


def pack(scaled, noise):
    n, feat = scaled.shape
    groups, per, tiles = layout(n, feat)
    lane = lax.broadcasted_iota(jnp.int32, (8, feat), 1)
    levels = jnp.zeros((8, feat), jnp.float32)
    for g in range(groups):
        levels = jnp.where(lane == g, noise[8 * g : 8 * g + 8, :feat], levels)
    pieces = [scaled[8 * g : 8 * g + 8] for g in range(groups)] + [levels]
    pieces += [jnp.zeros((8, feat), jnp.float32)] * (per * tiles - groups - 1)
    return jnp.concatenate(
        [jnp.concatenate(pieces[per * t : per * (t + 1)], axis=1) for t in range(tiles)], axis=0
    )


def unpack(packed, n, feat):
    groups, per, tiles = layout(n, feat)
    pieces = []
    for first in range(0, packed.shape[0], 8 * tiles):
        for g in range(groups):
            at, lane = first + 8 * (g // per), feat * (g % per)
            pieces.append(packed[at : at + 8, lane : lane + feat])
    return jnp.concatenate(pieces, axis=0)


def gather_kernel(
    dims, points, ids, shift, level, w_in, b_in, w_out, inv_scale, direction,
    feat_all, dir_col, own, row_feat, col_feat, send_sem, recv_sem,
):
    peers = Peers(*dims)
    rows, cols = dims
    n, feat = points.shape[0], w_out.shape[0]
    high = 8 * layout(n, feat)[2]
    r, c = lax.axis_index("row"), lax.axis_index("col")
    peers.greet()
    scaled, noise = features(
        points[...], ids[...], shift[...], level[...], w_in[...], b_in[...], w_out[...], inv_scale[...]
    )
    mine = pl.ds(pl.multiple_of(peers.me * high, 8), high)
    feat_all[mine, :] = pack(scaled, noise)
    own[...] = jnp.concatenate([scaled, noise[:, feat:]], axis=1)
    block = pl.ds(pl.multiple_of(r * n, 8), n)
    dir_col[block, :] = direction[...]
    peers.meet()
    peers.each(
        lambda t, dev: peers.send(
            feat_all.at[mine], feat_all.at[mine], send_sem.at[0], recv_sem.at[0], dev
        )
    )

    def turn(d, carry):
        dev = {"row": lax.rem(r + d, rows), "col": c}
        peers.send(direction, dir_col.at[block], send_sem.at[1], recv_sem.at[1], dev)
        return carry

    lax.fori_loop(1, rows, turn, 0)
    others = pl.ds(0, (peers.count - 1) * high)
    other_rows = pl.ds(0, (rows - 1) * n)
    take(feat_all.at[others], recv_sem.at[0])
    row_feat[...] = feat_all[pl.ds(pl.multiple_of(r * (cols * high), 8), cols * high), :]
    for q in range(rows):
        col_feat[q * high : (q + 1) * high, :] = feat_all[
            pl.ds(pl.multiple_of((q * cols + c) * high, 8), high), :
        ]
    take(dir_col.at[other_rows], recv_sem.at[1])
    take(feat_all.at[others], send_sem.at[0])
    take(dir_col.at[other_rows], send_sem.at[1])


def local_kernel(
    n, feat_all, dir_col, row_feat, col_feat, own, freq, phase, inverse, capacity, partial, basis_own
):
    feat, rank = freq.shape
    groups, per, tiles = layout(n, feat)
    amp = math.sqrt(2.0 / rank)
    count = feat_all.shape[0] // (8 * tiles)
    diag = lax.broadcasted_iota(jnp.int32, (rank, rank), 0) == lax.broadcasted_iota(
        jnp.int32, (rank, rank), 1
    )
    capacity[...] = jnp.where(diag, 1.0, 0.0)
    view = feat_all[...].reshape(count, tiles, 8, 128)
    levels = view[:, groups // per].reshape(count * 8, 128)
    first = feat * (groups % per)
    for g in range(groups):
        block = view[:, g // per].reshape(count * 8, 128)
        above, below = feat * (g % per), 128 - feat * (g % per + 1)
        wide = [freq[...]]
        if above:
            wide.insert(0, jnp.zeros((above, rank), jnp.float32))
        if below:
            wide.append(jnp.zeros((below, rank), jnp.float32))
        basis = amp * cosine(mm(block, jnp.concatenate(wide, axis=0)) + phase[...])
        capacity[...] += mm(basis, basis / levels[:, first + g : first + g + 1], 0, 0)
    basis_own[...] = amp * cosine(mm(own[...][:, :feat], freq[...]) + phase[...])
    over = unpack(row_feat[...], n, feat)
    under = unpack(col_feat[...], n, feat)
    sq_over = jnp.sum(over * over, axis=1, keepdims=True)
    sq_under = mm(jnp.ones((8, feat), jnp.float32), under * under, 1, 1)[0:1, :]
    distance = sq_over + sq_under - 2.0 * mm(over, under, 1, 1)
    partial[...] = mm(jnp.exp(-0.5 * distance), dir_col[...])
    inverse[...] = invert(capacity[...])


def reduce_kernel(
    dims, owners, own, partial, direction, residual, basis, prior,
    sums, projected, image,
    sums_all, part, slots, blocks, send_sem, recv_sem,
):
    peers = Peers(*dims)
    me, count = peers.me, peers.count
    cols = dims[1]
    n, rhs = direction.shape
    r, c = lax.axis_index("row"), lax.axis_index("col")
    peers.greet()
    noise = own[...][:, 127:128]
    res, d = residual[...], direction[...]
    sres = res / noise
    block = pl.ds(pl.multiple_of(c * n, 8), n)
    blocks[block, :] = partial[block, :]
    peers.meet()

    def turn(k, carry):
        t = lax.rem(c + k, cols)
        peers.send(
            partial.at[pl.ds(pl.multiple_of(t * n, 8), n)],
            blocks.at[block], send_sem.at[3], recv_sem.at[3], {"row": r, "col": t},
        )
        return carry

    lax.fori_loop(1, cols, turn, 0)
    rank = projected.shape[0]
    rq = rank // owners
    proj_res = mm(basis[...], sres, 0, 0).reshape(owners, 1, rq, rhs)
    other_cols = pl.ds(0, (cols - 1) * n)
    take(blocks.at[other_cols], recv_sem.at[3])
    img = jnp.sum(blocks[...].reshape(cols, n, rhs), axis=0) + noise * d
    image[...] = img
    simg = img / noise
    mine = pl.ds(pl.multiple_of(me * 8, 8), 8)
    sums_all[mine, :] = jnp.concatenate(
        [
            jnp.sum(d * img, axis=0, keepdims=True),
            jnp.sum(res * sres, axis=0, keepdims=True),
            jnp.sum(res * simg, axis=0, keepdims=True),
            jnp.sum(img * simg, axis=0, keepdims=True),
            jnp.zeros((4, rhs), jnp.float32),
        ],
        axis=0,
    )
    proj_img = mm(basis[...], simg, 0, 0).reshape(owners, 1, rq, rhs)
    part[...] = jnp.concatenate([proj_res, proj_img], axis=1).reshape(2 * rank, rhs)
    slot = pl.ds(pl.multiple_of(me * (2 * rq), 8), 2 * rq)

    def scatter(t, dev):
        def go():
            peers.send(
                part.at[pl.ds(pl.multiple_of(t * (2 * rq), 8), 2 * rq)],
                slots.at[slot], send_sem.at[1], recv_sem.at[1], dev,
            )

        peers.send(sums_all.at[mine], sums_all.at[mine], send_sem.at[0], recv_sem.at[0], dev)
        if owners < count:
            pl.when(t < owners)(go)
        else:
            go()

    peers.each(scatter)
    other_sums = pl.ds(0, (count - 1) * 8)
    take(sums_all.at[other_sums], recv_sem.at[0])
    totals = jnp.sum(sums_all[...].reshape(count, 8, rhs), axis=0)
    sums[...] = totals
    alpha = prior[...] / totals[0:1, :]

    def owner():
        result = pl.ds(pl.multiple_of(me * rq, 8), rq)
        slots[slot, :] = part[slot, :]
        take(slots.at[pl.ds(0, (count - 1) * 2 * rq)], recv_sem.at[1])
        both = jnp.sum(slots[...].reshape(count, 2 * rq, rhs), axis=0)
        projected[result, :] = both[:rq] - alpha * both[rq:]
        if owners > 1:
            take(part.at[pl.ds(0, (owners - 1) * 2 * rq)], send_sem.at[1])
        peers.each(
            lambda t, dev: peers.send(
                projected.at[result], projected.at[result], send_sem.at[2], recv_sem.at[2], dev
            )
        )
        if owners > 1:
            take(projected.at[pl.ds(0, (owners - 1) * rq)], recv_sem.at[2])
        take(slots.at[pl.ds(0, (count - 1) * rq)], send_sem.at[2])

    def guest():
        take(projected, recv_sem.at[2])
        take(part, send_sem.at[1])

    if owners < count:
        pl.when(me < owners)(owner)
        pl.when(me >= owners)(guest)
    else:
        owner()
    take(sums_all.at[other_sums], send_sem.at[0])
    take(blocks.at[other_cols], send_sem.at[3])


def final_kernel(
    inverse, capacity, projected, sums, own, image, direction, residual, sol, basis, prior,
    new_sol, new_res, new_dir, new_prod,
):
    proj, tot = projected[...], sums[...]
    alpha = prior[...] / tot[0:1, :]
    coeffs = mm(inverse[...], proj)
    coeffs = coeffs + mm(inverse[...], proj - mm(capacity[...], coeffs))
    noise = own[...][:, 127:128]
    d = direction[...]
    nres = residual[...] - alpha * image[...]
    norm = tot[1:2, :] - 2.0 * alpha * tot[2:3, :] + alpha * alpha * tot[3:4, :]
    prod = norm - jnp.sum(proj * coeffs, axis=0, keepdims=True)
    precond = (nres - mm(basis[...], coeffs)) / noise
    new_sol[...] = sol[...] + alpha * d
    new_res[...] = nres
    new_dir[...] = precond + prod / prior[...] * d
    new_prod[...] = prod


def per_device(
    dims, points, source_ids, source_shift, noise_level, weight_in, bias_in, weight_out,
    inverse_scale, frequency, phase_shift, solution, residual, direction, prior_product,
):
    count = dims[0] * dims[1]
    n, rhs = direction.shape
    feat, rank = frequency.shape
    f32 = jnp.float32
    sds = jax.ShapeDtypeStruct
    row = lambda v: v.reshape(1, -1)
    dma = pltpu.SemaphoreType.DMA
    prior = row(prior_product)
    high = 8 * layout(n, feat)[2]
    feat_all, dir_col, own, row_feat, col_feat = pl.pallas_call(
        functools.partial(gather_kernel, dims),
        out_shape=(
            sds((count * high, 128), f32), sds((dims[0] * n, rhs), f32), sds((n, 128), f32),
            sds((dims[1] * high, 128), f32), sds((dims[0] * high, 128), f32),
        ),
        in_specs=[VMEM] * 9,
        out_specs=(VMEM,) * 5,
        scratch_shapes=[dma((2,)), dma((2,))],
        compiler_params=pltpu.CompilerParams(collective_id=0, has_side_effects=True),
        name="gather",
    )(
        points, row(source_ids), source_shift, row(noise_level), weight_in, row(bias_in),
        weight_out.T, row(inverse_scale), direction,
    )
    phase = row(phase_shift)
    square = sds((rank, rank), f32)
    inverse, capacity, partial, basis = pl.pallas_call(
        functools.partial(local_kernel, n),
        out_shape=(square, square, sds((dims[1] * n, rhs), f32), sds((n, rank), f32)),
        in_specs=[VMEM] * 7,
        out_specs=(VMEM,) * 4,
        name="local",
    )(feat_all, dir_col, row_feat, col_feat, own, frequency, phase)
    owners = min(count, rank // 8)
    sums, projected, image = pl.pallas_call(
        functools.partial(reduce_kernel, dims, owners),
        out_shape=(sds((8, rhs), f32), sds((rank, rhs), f32), sds((n, rhs), f32)),
        in_specs=[VMEM] * 6,
        out_specs=(VMEM,) * 3,
        scratch_shapes=[
            pltpu.VMEM((8 * count, rhs), f32),
            pltpu.VMEM((2 * rank, rhs), f32),
            pltpu.VMEM((count * (2 * rank // owners), rhs), f32),
            pltpu.VMEM((dims[1] * n, rhs), f32),
            dma((4,)),
            dma((4,)),
        ],
        compiler_params=pltpu.CompilerParams(collective_id=1, has_side_effects=True),
        name="reduce",
    )(own, partial, direction, residual, basis, prior)
    block = sds((n, rhs), f32)
    new_sol, new_res, new_dir, new_prod = pl.pallas_call(
        final_kernel,
        out_shape=(block, block, block, sds((1, rhs), f32)),
        in_specs=[VMEM] * 11,
        out_specs=(VMEM,) * 4,
        name="final",
    )(inverse, capacity, projected, sums, own, image, direction, residual, solution, basis, prior)
    return new_sol, new_res, new_dir, new_prod.reshape(rhs)


BF16 = jnp.bfloat16


def dot(a, b, ca=1, cb=0):
    return lax.dot_general(a, b, (((ca,), (cb,)), ((), ())), preferred_element_type=jnp.float32)


def split(x):
    high = x.astype(BF16)
    rest = x - high.astype(jnp.float32)
    mid = rest.astype(BF16)
    low = (rest - mid.astype(jnp.float32)).astype(BF16)
    return high, mid, low


def rows_of(x):
    parts = [p.astype(jnp.float32) for p in split(x)]
    fill = -3 * x.shape[0] % 16
    if fill:
        parts.append(jnp.zeros((fill, x.shape[1]), jnp.float32))
    return jnp.concatenate(parts, axis=0).astype(BF16)


def fold(acc, q):
    return acc[0:q] + acc[q : 2 * q] + acc[2 * q : 3 * q]


def iota(shape, dim):
    return lax.broadcasted_iota(jnp.int32, shape, dim)


def pivot_inverse(at):
    a00, a01, a11 = at(0, 0), at(0, 1), at(1, 1)
    b00, b01, b10, b11 = at(0, 2), at(0, 3), at(1, 2), at(1, 3)
    d00, d01, d11 = at(2, 2), at(2, 3), at(3, 3)
    inv = 1.0 / (a00 * a11 - a01 * a01)
    e00, e01, e11 = a11 * inv, -a01 * inv, a00 * inv
    f00, f01 = e00 * b00 + e01 * b10, e00 * b01 + e01 * b11
    f10, f11 = e01 * b00 + e11 * b10, e01 * b01 + e11 * b11
    s00 = d00 - (b00 * f00 + b10 * f10)
    s01 = d01 - (b00 * f01 + b10 * f11)
    s11 = d11 - (b01 * f01 + b11 * f11)
    inv = 1.0 / (s00 * s11 - s01 * s01)
    t00, t01, t11 = s11 * inv, -s01 * inv, s00 * inv
    g00, g01 = f00 * t00 + f01 * t01, f00 * t01 + f01 * t11
    g10, g11 = f10 * t00 + f11 * t01, f10 * t01 + f11 * t11
    p00 = e00 + g00 * f00 + g01 * f01
    p01 = e01 + g00 * f10 + g01 * f11
    p11 = e11 + g10 * f10 + g11 * f11
    return (
        (p00, p01, -g00, -g01),
        (p01, p11, -g10, -g11),
        (-g00, -g10, t00, t01),
        (-g01, -g11, t01, t11),
    )


def column(m, at):
    lane = lax.broadcasted_iota(jnp.int32, m.shape, 1)
    return jnp.broadcast_to(jnp.sum(jnp.where(lane == at, m, 0.0), axis=1, keepdims=True), m.shape)


def sweep(rows, first):
    size, wide = rows.shape
    groups, tiles = size // 8, wide // 128
    full = (8, 128)
    m = [[rows[8 * g : 8 * g + 8, t * 128 : (t + 1) * 128] for t in range(tiles)] for g in range(groups)]
    lane = lax.broadcasted_iota(jnp.int32, full, 1)
    sub = lax.broadcasted_iota(jnp.int32, full, 0)

    def line(x, i):
        return jnp.broadcast_to(x[i : i + 1, :], full)

    def columns(row, k):
        home, at0 = divmod(first + k, 128)
        return [column(row[home], at0 + j) for j in range(4)]

    near = columns(m[0], 0)
    for k in range(0, size, 4):
        group, off = divmod(k, 8)
        home, at0 = divmod(first + k, 128)
        cols = [columns(m[g], k) for g in range(groups)]
        pivots = pivot_inverse(lambda i, j: line(near[j], off + i))
        if k + 4 < size:
            after = (k + 4) // 8
            ahead = columns(m[after], k + 4)
            other = ahead if after == group else columns(m[group], k + 4)
            past = [[line(other[j], off + l) for l in range(4)] for j in range(4)]
            c = cols[after]
            gain = [
                (c[0] * pivots[0][l] + c[1] * pivots[1][l]) + (c[2] * pivots[2][l] + c[3] * pivots[3][l])
                for l in range(4)
            ]
            near = [
                ahead[j]
                - ((gain[0] * past[j][0] + gain[1] * past[j][1]) + (gain[2] * past[j][2] + gain[3] * past[j][3]))
                for j in range(4)
            ]
        inside = (lane >= at0) & (lane < at0 + 4)
        out = [[None] * tiles for _ in range(groups)]
        for t in range(tiles):
            own = [line(m[group][t], off + l) for l in range(4)]
            if t == home:
                own = [
                    jnp.where(lane == at0 + l, 1.0, jnp.where(inside, 0.0, own[l])) for l in range(4)
                ]
            scaled = [(p[0] * own[0] + p[1] * own[1]) + (p[2] * own[2] + p[3] * own[3]) for p in pivots]
            for g in range(groups):
                base = jnp.where(inside, 0.0, m[g][t]) if t == home else m[g][t]
                c = cols[g]
                x = base - (
                    (c[0] * scaled[0] + c[1] * scaled[1]) + (c[2] * scaled[2] + c[3] * scaled[3])
                )
                if g == group:
                    for l in range(4):
                        x = jnp.where(sub == off + l, scaled[l], x)
                out[g][t] = x
        m = out
    return jnp.concatenate([jnp.concatenate(r, axis=1) for r in m], axis=0)


def exact(a, b):
    ah, am, al = split(a)
    bh, bm, bl = split(b)
    return dot(ah, bh) + (dot(ah, bm) + dot(am, bh)) + (dot(am, bm) + dot(ah, bl) + dot(al, bh))


def invert_panels(a):
    size = a.shape[0]
    step = min(128, size)
    lane = iota((1, size), 1)
    for k in range(0, size, step):
        rows = sweep(a[k : k + step], k)
        pieces = [(k, rows)]
        for lo, hi in ((0, k), (k + step, size)):
            if hi > lo:
                part = a[lo:hi]
                base = jnp.where((lane >= k) & (lane < k + step), 0.0, part)
                pieces.append((lo, base - exact(part[:, k : k + step], rows)))
        pieces.sort(key=lambda v: v[0])
        a = jnp.concatenate([p for _, p in pieces], axis=0) if len(pieces) > 1 else rows
    return a


class Plan:
    def __init__(self, dims, n, rhs, feat):
        self.count = dims[0] * dims[1]
        self.pairs = self.count // 2
        self.n, self.rhs, self.feat = n, rhs, feat
        self.q = rhs // self.pairs
        self.per = 128 // n
        self.windows = -(-self.count // self.per)
        self.wide = 128 * self.windows
        self.groups = n // 8
        self.pieces = 128 // feat - 1
        self.tiles = -(-self.groups // self.pieces)
        self.even = dims[0] % 2 == 0

    def fits(self):
        return (
            self.even
            and self.rhs == 128
            and self.q == 8
            and 2 * self.n + 1 <= 128
            and self.per * self.n < 128
            and self.n % 8 == 0
            and self.groups <= 8
            and self.feat % 16 == 0
            and self.feat <= 32
            and self.wide <= 2048
        )


def cosine_turns(u):
    r = u - jnp.round(u)
    z = r * r
    p = SIN[-1]
    for c in SIN[-2::-1]:
        p = p * z + c
    s = p * r
    return 1.0 - 2.0 * (s * s)


SIN = tuple((-1.0) ** i * math.pi ** (2 * i + 1) / math.factorial(2 * i + 1) for i in range(7))


def pack_tiles(plan, scaled, noise):
    feat = plan.feat
    lane = iota((8, feat), 1)
    levels = jnp.zeros((8, feat), jnp.float32)
    for g in range(plan.groups):
        levels = jnp.where(lane == g, noise[8 * g : 8 * g + 8, :feat], levels)
    tiles = []
    for t in range(plan.tiles):
        row = []
        for j in range(plan.pieces):
            g = t * plan.pieces + j
            row.append(
                scaled[8 * g : 8 * g + 8] if g < plan.groups else jnp.zeros((8, feat), jnp.float32)
            )
        tiles.append(jnp.concatenate(row + [levels], axis=1))
    return tiles


def unpack_tiles(plan, feat_all):
    n, feat, per = plan.n, plan.feat, plan.per
    group = lax.rem(iota((8, 128), 1), n) // 8
    place = lax.rem(group, plan.pieces)[0:1]
    zero = jnp.zeros((8, 128), jnp.float32)
    features, levels = [], []
    for w in range(plan.windows):
        rows = []
        for k in range(per):
            s = w * per + k
            for g in range(plan.groups):
                rows.append(feat_all[s // plan.pairs, s % plan.pairs, g // plan.pieces] if s < plan.count else zero)
        rows += [zero] * (16 - len(rows))
        turned = jnp.concatenate(rows, axis=0).T
        out = turned[(plan.pieces - 1) * feat : plan.pieces * feat]
        for j in range(plan.pieces - 1):
            out = jnp.where(place == j, turned[j * feat : (j + 1) * feat], out)
        features.append(out)
        base = plan.pieces * feat
        level = jnp.where(iota((8, 128), 0) == group, turned[base : base + 8], 0.0)
        levels.append(jnp.sum(level, axis=0, keepdims=True))
    return jnp.concatenate(features, axis=1), jnp.concatenate(levels, axis=1)


def live_lanes(plan):
    lane = iota((1, plan.wide), 1)
    inside = lax.rem(lane, 128)
    source = (lane // 128) * plan.per + inside // plan.n
    return (inside < plan.per * plan.n) & (source < plan.count)


def between(lane, start, n):
    first = start % 128
    last = first + n
    if last <= 128:
        return (lane >= first) & (lane < last)
    return (lane >= first) | (lane < last - 128)


def main_kernel(
    dims, points, ids, shift, level, w_in, b_in, w_out, inv_scale, freq, phase,
    residual, direction, prior,
    res_all, dir_all,
    feat_all, turned, slabs, right, left, capacity, inverse, basis, passed, stage, send_sem, recv_sem,
):
    peers = Peers(*dims)
    rows, cols = dims
    n, rhs = direction.shape
    feat, rank = freq.shape
    plan = Plan(dims, n, rhs, feat)
    count, pairs, q, per = plan.count, plan.pairs, plan.q, plan.per
    wide, windows = plan.wide, plan.windows
    r, c = lax.axis_index("row"), lax.axis_index("col")
    half = lax.rem(r, 2)
    pair = (r // 2) * cols + c
    me = half * pairs + pair
    f32 = jnp.float32

    def device(h, p):
        return {"row": 2 * (p // cols) + h, "col": lax.rem(p, cols)}

    sibling = {"row": 2 * (r // 2) + (1 - half), "col": c}

    def loop(first, body):
        def step(i, carry):
            body(lax.rem(pair + i, pairs))
            return carry

        lax.fori_loop(first, pairs, step, 0)

    peers.greet()
    scaled, noise = features(
        points[...], ids[...], shift[...], level[...], w_in[...], b_in[...], w_out[...], inv_scale[...]
    )
    for t, tile in enumerate(pack_tiles(plan, scaled, noise)):
        feat_all[half, pair, t] = tile
    peers.meet()
    mine = feat_all.at[half, pair]
    loop(1, lambda p: peers.send(mine, mine, send_sem.at[0], recv_sem.at[0], device(half, p)))
    stacked = jnp.concatenate(
        [direction[...], residual[...], prior[...], jnp.zeros((127 - 2 * n, rhs), f32)], axis=0
    )
    spun = pltpu.roll(stacked.T, n * lax.rem(me, per), 1)
    for p in range(pairs):
        turned[p] = spun[p * q : (p + 1) * q]

    def give(p):
        peers.send(turned.at[p], slabs.at[me], send_sem.at[2], recv_sem.at[2], device(0, p))

    loop(1, give)

    @pl.when(half == 1)
    def _():
        give(pair)

    @pl.when(half == 0)
    def _():
        slabs[me] = turned[pair]

    turn = 1.0 / (2.0 * math.pi)
    both = jnp.concatenate([freq[...], phase[...], jnp.zeros((127 - feat, rank), f32)], axis=0) * turn
    fp = both.T
    fh, fm, fl = [p.astype(f32) for p in split(fp)]
    fills = 256 - 6 * feat - 3
    spectral = jnp.concatenate(
        [fh[:, :feat], fh[:, :feat], fh[:, :feat], fm[:, :feat], fm[:, :feat], fl[:, :feat]]
        + [p[:, feat : feat + 1] for p in (fh, fm, fl)]
        + [jnp.zeros((rank, fills), f32)],
        axis=1,
    ).astype(BF16)
    lane = iota((1, 128), 1)
    live = live_lanes(plan)

    take(feat_all.at[0, pl.ds(0, pairs - 1)], recv_sem.at[0])
    peers.send(feat_all.at[half], feat_all.at[half], send_sem.at[1], recv_sem.at[1], sibling)
    take(feat_all.at[0], recv_sem.at[1])
    ft, levels = unpack_tiles(plan, feat_all)
    levels = jnp.where(live, levels, 1.0)
    rsn = jnp.where(live, lax.rsqrt(levels), 0.0)
    h, m, l = split(ft)
    ft2 = ft * math.log2(math.e)
    sq = -0.5 * jnp.sum(ft2 * ft, axis=0, keepdims=True)
    sqs = [p.astype(f32) for p in split(sq)]
    ones = jnp.ones((3, wide), f32)
    rest = jnp.zeros((256 - 6 * feat - 6, wide), f32)
    right[...] = jnp.concatenate(
        [h, m, l, h, m, h, jnp.concatenate([ones] + sqs + [rest], axis=0).astype(BF16)], axis=0
    )
    amp = math.sqrt(2.0 / rank)
    u = dot(spectral, right[...])
    ch, cm, cl = split(cosine_turns(u) * (amp * rsn))
    basis[0] = ch
    basis[1] = cm
    basis[2] = cl
    tail = lane >= per * n

    @pl.when(half == 0)
    def _():
        h2, m2, l2 = split(ft2)
        low = jnp.concatenate(
            [h2, h2, h2, m2, m2, l2, jnp.concatenate(sqs + [ones, rest], axis=0).astype(BF16)], axis=0
        )
        left[...] = low.T
        take(slabs.at[pl.ds(0, count - 1)], recv_sem.at[2])
        zero = jnp.zeros((q, 128), f32)
        dirs, ress = [], []
        for w in range(windows):
            own = [slabs[w * per + k] if w * per + k < count else zero for k in range(per)]
            d, x = zero, zero
            for k in range(per):
                d = jnp.where(between(lane, k * n, n), own[k], d)
                x = jnp.where(between(lane, (k + 1) * n, n), own[k], x)
            dirs.append(d)
            ress.append(pltpu.roll(x, 128 - n, 1))
        d = jnp.concatenate(dirs, axis=1)
        res = jnp.concatenate(ress, axis=1)
        spin = pltpu.roll(slabs[me], lax.rem(128 - n * lax.rem(me, per), 128), 1)
        own_prior = spin[:, 2 * n : 2 * n + 1]
        d3 = rows_of(d)
        acc = jnp.zeros((d3.shape[0], wide), f32)
        for w in range(windows):
            k = jnp.exp2(dot(left[w * 128 : (w + 1) * 128, :], right[...]))
            kh = k.astype(BF16)
            kl = (k - kh.astype(f32)).astype(BF16)
            part = d3[:, w * 128 : (w + 1) * 128]
            acc = acc + (dot(part, kh) + dot(part, kl))
        img = fold(acc, q) + levels * d
        alpha = own_prior / jnp.sum(d * img, axis=1, keepdims=True)
        nres = res - alpha * img
        y = nres * rsn
        y3 = rows_of(y)
        proj = fold(
            dot(y3, basis[0], 1, 1) + dot(y3, basis[1], 1, 1) + dot(y3, basis[2], 1, 1), q
        )
        for w in range(windows):
            at = slice(w * 128, (w + 1) * 128)
            stage[w] = jnp.where(tail, alpha, nres[:, at])
            passed[w] = d[:, at]
            passed[windows + w] = y[:, at]
        for w in range(rank // 128):
            passed[2 * windows + w] = proj[:, w * 128 : (w + 1) * 128]
        passed[2 * windows + rank // 128] = jnp.broadcast_to(own_prior, (q, 128))
        peers.send(passed, passed, send_sem.at[3], recv_sem.at[3], sibling)
        res_all[pair] = stage[me // per]

        def give_rest(h, p):
            s = h * pairs + p
            peers.send(stage.at[s // per], res_all.at[pair], send_sem.at[4], recv_sem.at[4], device(h, p))

        loop(1, lambda p: give_rest(0, p))
        loop(0, lambda p: give_rest(1, p))

    @pl.when(half == 1)
    def _():
        diag = iota((rank, rank), 0) == iota((rank, rank), 1)
        cross = dot(ch, cm, 1, 1) + dot(ch, cl, 1, 1)
        capacity[...] = (
            jnp.where(diag, 1.0, 0.0) + (dot(ch, ch, 1, 1) + dot(cm, cm, 1, 1)) + (cross + cross.T)
        )
        inverse[...] = invert_panels(capacity[...])
        take(passed, recv_sem.at[3])
        proj = jnp.concatenate([passed[2 * windows + w] for w in range(rank // 128)], axis=1)
        coeffs = mm(proj, inverse[...])
        coeffs = coeffs + mm(proj - mm(coeffs, capacity[...]), inverse[...])
        c3 = rows_of(coeffs)
        back = fold(dot(c3, basis[0]) + dot(c3, basis[1]) + dot(c3, basis[2]), q)
        d = jnp.concatenate([passed[w] for w in range(windows)], axis=1)
        y = jnp.concatenate([passed[windows + w] for w in range(windows)], axis=1)
        own_prior = passed[2 * windows + rank // 128][:, 0:1]
        gap = y - back
        prod = jnp.sum(y * gap, axis=1, keepdims=True)
        ndir = gap * rsn + prod / own_prior * d
        for w in range(windows):
            stage[w] = jnp.where(tail, prod, ndir[:, w * 128 : (w + 1) * 128])
        dir_all[pair] = stage[me // per]

        def give_dir(h, p):
            s = h * pairs + p
            peers.send(stage.at[s // per], dir_all.at[pair], send_sem.at[4], recv_sem.at[5], device(h, p))

        loop(1, lambda p: give_dir(1, p))
        loop(0, lambda p: give_dir(0, p))

    @pl.when(half == 0)
    def _():
        take(slabs.at[pl.ds(0, pairs - 1)], send_sem.at[2])
        take(passed, send_sem.at[3])
        take(res_all.at[pl.ds(0, pairs - 1)], recv_sem.at[4])
        take(dir_all, recv_sem.at[5])

    @pl.when(half == 1)
    def _():
        take(slabs.at[pl.ds(0, pairs)], send_sem.at[2])
        take(res_all, recv_sem.at[4])
        take(dir_all.at[pl.ds(0, pairs - 1)], recv_sem.at[5])

    take(feat_all.at[0, pl.ds(0, pairs - 1)], send_sem.at[0])
    take(feat_all.at[0], send_sem.at[1])
    take(slabs.at[pl.ds(0, count - 1)], send_sem.at[4])


def finish_kernel(dims, res, dirs, direction, sol, new_sol, new_res, new_dir, new_prod, spare):
    r, c = lax.axis_index("row"), lax.axis_index("col")
    me = lax.rem(r, 2) * (dims[0] * dims[1] // 2) + (r // 2) * dims[1] + c
    n = direction.shape[0]
    own = pl.ds(pl.multiple_of(n * lax.rem(me, 128 // n), 8), n)
    x = res[...].T
    spare[...] = x
    new_res[...] = spare[own, :]
    new_sol[...] = sol[...] + x[127:128] * direction[...]
    z = dirs[...].T
    spare[...] = z
    new_dir[...] = spare[own, :]
    new_prod[...] = z[127:128]


def per_device_columns(
    dims, points, source_ids, source_shift, noise_level, weight_in, bias_in, weight_out,
    inverse_scale, frequency, phase_shift, solution, residual, direction, prior_product,
):
    n, rhs = direction.shape
    feat, rank = frequency.shape
    plan = Plan(dims, n, rhs, feat)
    count, pairs, q, wide, windows = plan.count, plan.pairs, plan.q, plan.wide, plan.windows
    f32 = jnp.float32
    sds = jax.ShapeDtypeStruct
    row = lambda v: v.reshape(1, -1)
    dma = pltpu.SemaphoreType.DMA
    res, dirs = pl.pallas_call(
        functools.partial(main_kernel, dims),
        out_shape=(sds((pairs, q, 128), f32), sds((pairs, q, 128), f32)),
        in_specs=[VMEM] * 13,
        out_specs=(VMEM,) * 2,
        scratch_shapes=[
            pltpu.VMEM((2, pairs, plan.tiles, 8, 128), f32),
            pltpu.VMEM((pairs, q, 128), f32),
            pltpu.VMEM((count, q, 128), f32),
            pltpu.VMEM((256, wide), BF16),
            pltpu.VMEM((wide, 256), BF16),
            pltpu.VMEM((rank, rank), f32),
            pltpu.VMEM((rank, rank), f32),
            pltpu.VMEM((3, rank, wide), BF16),
            pltpu.VMEM((2 * windows + rank // 128 + 1, q, 128), f32),
            pltpu.VMEM((windows, q, 128), f32),
            dma((6,)),
            dma((6,)),
        ],
        compiler_params=pltpu.CompilerParams(collective_id=0, has_side_effects=True),
        name="columns",
    )(
        points, row(source_ids), source_shift, row(noise_level), weight_in, row(bias_in),
        weight_out.T, row(inverse_scale), frequency, row(phase_shift), residual, direction,
        row(prior_product),
    )
    block = sds((n, rhs), f32)
    new_sol, new_res, new_dir, new_prod = pl.pallas_call(
        functools.partial(finish_kernel, dims),
        out_shape=(block, block, block, sds((1, rhs), f32)),
        in_specs=[VMEM] * 4,
        out_specs=(VMEM,) * 4,
        scratch_shapes=[pltpu.VMEM((128, rhs), f32)],
        name="finish",
    )(res.reshape(rhs, 128), dirs.reshape(rhs, 128), direction, solution)
    return new_sol, new_res, new_dir, new_prod.reshape(rhs)


def dispatch(dims, *args):
    n, rhs = args[12].shape
    feat = args[8].shape[0]
    if Plan(dims, n, rhs, feat).fits():
        return per_device_columns(dims, *args)
    return per_device(dims, *args)


def solution(mesh):
    dims = (mesh.shape["row"], mesh.shape["col"])
    rows = P(("row", "col"), None)
    in_specs = (
        rows, P(("row", "col")), P(), P(), P(), P(), P(), P(), P(), P(), rows, rows, rows, P(),
    )
    return jax.shard_map(
        functools.partial(dispatch, dims),
        mesh=mesh,
        in_specs=in_specs,
        out_specs=(rows, rows, rows, P()),
        check_vma=False,
    )
```

```python
import functools
import math

import jax
import jax.numpy as jnp
from jax import lax
from jax.experimental import pallas as pl
from jax.experimental.pallas import tpu as pltpu
from jax.sharding import PartitionSpec as P
HIGH = lax.Precision.HIGHEST
MESH = pl.DeviceIdType.MESH
VMEM = pl.BlockSpec(memory_space=pltpu.VMEM)


def mm(a, b, ca=1, cb=0):
    return lax.dot_general(
        a, b, (((ca,), (cb,)), ((), ())), precision=HIGH, preferred_element_type=jnp.float32
    )


def cosine(x):
    n = jnp.floor(x * 0.3183098861837907 + 0.5)
    r = ((x - n * 3.140625) - n * 9.67502593994140625e-4) - n * 1.509957990978376432e-7
    half = n * 0.5
    sign = 1.0 - 4.0 * (half - jnp.floor(half))
    z = r * r
    p = 2.08767569878681e-9
    for c in (
        -2.75573192239859e-7,
        2.48015873015873e-5,
        -1.38888888888889e-3,
        4.16666666666667e-2,
        -0.5,
        1.0,
    ):
        p = p * z + c
    return sign * p


def invert_block(m):
    size = m.shape[0]
    m = m.reshape(size // 8, 8, size)
    shape = m.shape
    lane = lax.broadcasted_iota(jnp.int32, (8, size), 1)
    sub = lax.broadcasted_iota(jnp.int32, (8, size), 0)
    for k in range(0, size, 4):
        group, off = divmod(k, 8)
        cols = [jnp.broadcast_to(m[:, :, k + j : k + j + 1], shape) for j in range(4)]
        own = m[group]
        rows = [jnp.broadcast_to(own[off + i : off + i + 1, :], (8, size)) for i in range(4)]

        def at(i, j):
            return jnp.broadcast_to(cols[j][group][off + i : off + i + 1, :], (8, size))

        a00, a01, a11 = at(0, 0), at(0, 1), at(1, 1)
        b00, b01, b10, b11 = at(0, 2), at(0, 3), at(1, 2), at(1, 3)
        d00, d01, d11 = at(2, 2), at(2, 3), at(3, 3)
        inv = 1.0 / (a00 * a11 - a01 * a01)
        e00, e01, e11 = a11 * inv, -a01 * inv, a00 * inv
        f00, f01 = e00 * b00 + e01 * b10, e00 * b01 + e01 * b11
        f10, f11 = e01 * b00 + e11 * b10, e01 * b01 + e11 * b11
        s00 = d00 - (b00 * f00 + b10 * f10)
        s01 = d01 - (b00 * f01 + b10 * f11)
        s11 = d11 - (b01 * f01 + b11 * f11)
        inv = 1.0 / (s00 * s11 - s01 * s01)
        t00, t01, t11 = s11 * inv, -s01 * inv, s00 * inv
        g00, g01 = f00 * t00 + f01 * t01, f00 * t01 + f01 * t11
        g10, g11 = f10 * t00 + f11 * t01, f10 * t01 + f11 * t11
        p00 = e00 + g00 * f00 + g01 * f01
        p01 = e01 + g00 * f10 + g01 * f11
        p11 = e11 + g10 * f10 + g11 * f11
        pivots = (
            (p00, p01, -g00, -g01),
            (p01, p11, -g10, -g11),
            (-g00, -g10, t00, t01),
            (-g01, -g11, t01, t11),
        )
        masks = [lane == k + j for j in range(4)]
        inside = (lane >= k) & (lane < k + 4)
        rows = [
            jnp.where(masks[j], 1.0, jnp.where(inside, 0.0, rows[j])) for j in range(4)
        ]
        scaled = [
            (pivots[i][0] * rows[0] + pivots[i][1] * rows[1])
            + (pivots[i][2] * rows[2] + pivots[i][3] * rows[3])
            for i in range(4)
        ]
        base = jnp.where(inside[None], 0.0, m)
        update = (cols[0] * scaled[0][None] + cols[1] * scaled[1][None]) + (
            cols[2] * scaled[2][None] + cols[3] * scaled[3][None]
        )
        m = base - update
        fixed = m[group]
        for i in range(4):
            fixed = jnp.where(sub == off + i, scaled[i], fixed)
        pieces = [fixed[None]]
        if group > 0:
            pieces.insert(0, m[:group])
        if group + 1 < size // 8:
            pieces.append(m[group + 1 :])
        m = jnp.concatenate(pieces, axis=0) if len(pieces) > 1 else pieces[0]
    return m.reshape(size, size)


def invert(a):
    size = a.shape[0]
    if size <= 128:
        return invert_block(a)
    h = size // 2
    top, cross, low = a[:h, :h], a[:h, h:], a[h:, h:]
    x = invert(top)
    y = mm(x, cross)
    z = invert(low - mm(cross, y, 0, 0))
    yz = mm(y, z)
    first = jnp.concatenate([x + mm(yz, y, 1, 1), -yz], axis=1)
    second = jnp.concatenate([-yz.T, z], axis=1)
    return jnp.concatenate([first, second], axis=0)


class Peers:
    def __init__(self, rows, cols):
        self.cols, self.count = cols, rows * cols
        self.me = lax.axis_index("row") * cols + lax.axis_index("col")

    def id(self, d):
        t = lax.rem(self.me + d, self.count)
        return t, {"row": t // self.cols, "col": lax.rem(t, self.cols)}

    def each(self, body):
        def turn(d, carry):
            body(*self.id(d))
            return carry

        lax.fori_loop(1, self.count, turn, 0)

    def greet(self):
        barrier = pltpu.get_barrier_semaphore()
        self.each(
            lambda t, dev: pl.semaphore_signal(barrier, inc=1, device_id=dev, device_id_type=MESH)
        )

    def meet(self):
        pl.semaphore_wait(pltpu.get_barrier_semaphore(), self.count - 1)

    def send(self, src, dst, send_sem, recv_sem, dev):
        pltpu.make_async_remote_copy(
            src_ref=src,
            dst_ref=dst,
            send_sem=send_sem,
            recv_sem=recv_sem,
            device_id=dev,
            device_id_type=MESH,
        ).start()


def take(ref, sem):
    pltpu.make_async_copy(ref, ref, sem).wait()


def features(points, ids, shift, level, w_in, b_in, w_out, inv_scale):
    n = points.shape[0]
    sources = shift.shape[0]
    onehot = (lax.broadcasted_iota(jnp.int32, (sources, n), 0) == ids).astype(jnp.float32)
    eye = lax.broadcasted_iota(jnp.int32, (sources, sources), 0) == lax.broadcasted_iota(
        jnp.int32, (sources, sources), 1
    )
    diag = jnp.where(eye, level, 0.0)
    spread = mm(diag, jnp.ones((sources, 128), jnp.float32))
    noise = mm(onehot, spread, 0, 0)
    shifted = points + mm(onehot, shift, 0, 0)
    hidden = jnp.tanh(mm(shifted, w_in) + b_in)
    scaled = mm(hidden, w_out, 1, 1) * inv_scale
    return scaled, noise


def layout(n, feat):
    groups, per = n // 8, 128 // feat
    return groups, per, -(-(groups + 1) // per)


def pack(scaled, noise):
    n, feat = scaled.shape
    groups, per, tiles = layout(n, feat)
    lane = lax.broadcasted_iota(jnp.int32, (8, feat), 1)
    levels = jnp.zeros((8, feat), jnp.float32)
    for g in range(groups):
        levels = jnp.where(lane == g, noise[8 * g : 8 * g + 8, :feat], levels)
    pieces = [scaled[8 * g : 8 * g + 8] for g in range(groups)] + [levels]
    pieces += [jnp.zeros((8, feat), jnp.float32)] * (per * tiles - groups - 1)
    return jnp.concatenate(
        [jnp.concatenate(pieces[per * t : per * (t + 1)], axis=1) for t in range(tiles)], axis=0
    )


def unpack(packed, n, feat):
    groups, per, tiles = layout(n, feat)
    pieces = []
    for first in range(0, packed.shape[0], 8 * tiles):
        for g in range(groups):
            at, lane = first + 8 * (g // per), feat * (g % per)
            pieces.append(packed[at : at + 8, lane : lane + feat])
    return jnp.concatenate(pieces, axis=0)


def gather_kernel(
    dims, points, ids, shift, level, w_in, b_in, w_out, inv_scale, direction,
    feat_all, dir_col, own, row_feat, col_feat, send_sem, recv_sem,
):
    peers = Peers(*dims)
    rows, cols = dims
    n, feat = points.shape[0], w_out.shape[0]
    high = 8 * layout(n, feat)[2]
    r, c = lax.axis_index("row"), lax.axis_index("col")
    peers.greet()
    scaled, noise = features(
        points[...], ids[...], shift[...], level[...], w_in[...], b_in[...], w_out[...], inv_scale[...]
    )
    mine = pl.ds(pl.multiple_of(peers.me * high, 8), high)
    feat_all[mine, :] = pack(scaled, noise)
    own[...] = jnp.concatenate([scaled, noise[:, feat:]], axis=1)
    block = pl.ds(pl.multiple_of(r * n, 8), n)
    dir_col[block, :] = direction[...]
    peers.meet()
    peers.each(
        lambda t, dev: peers.send(
            feat_all.at[mine], feat_all.at[mine], send_sem.at[0], recv_sem.at[0], dev
        )
    )

    def turn(d, carry):
        dev = {"row": lax.rem(r + d, rows), "col": c}
        peers.send(direction, dir_col.at[block], send_sem.at[1], recv_sem.at[1], dev)
        return carry

    lax.fori_loop(1, rows, turn, 0)
    others = pl.ds(0, (peers.count - 1) * high)
    other_rows = pl.ds(0, (rows - 1) * n)
    take(feat_all.at[others], recv_sem.at[0])
    row_feat[...] = feat_all[pl.ds(pl.multiple_of(r * (cols * high), 8), cols * high), :]
    for q in range(rows):
        col_feat[q * high : (q + 1) * high, :] = feat_all[
            pl.ds(pl.multiple_of((q * cols + c) * high, 8), high), :
        ]
    take(dir_col.at[other_rows], recv_sem.at[1])
    take(feat_all.at[others], send_sem.at[0])
    take(dir_col.at[other_rows], send_sem.at[1])


def local_kernel(
    n, feat_all, dir_col, row_feat, col_feat, own, freq, phase, inverse, capacity, partial, basis_own
):
    feat, rank = freq.shape
    groups, per, tiles = layout(n, feat)
    amp = math.sqrt(2.0 / rank)
    count = feat_all.shape[0] // (8 * tiles)
    diag = lax.broadcasted_iota(jnp.int32, (rank, rank), 0) == lax.broadcasted_iota(
        jnp.int32, (rank, rank), 1
    )
    capacity[...] = jnp.where(diag, 1.0, 0.0)
    view = feat_all[...].reshape(count, tiles, 8, 128)
    levels = view[:, groups // per].reshape(count * 8, 128)
    first = feat * (groups % per)
    for g in range(groups):
        block = view[:, g // per].reshape(count * 8, 128)
        above, below = feat * (g % per), 128 - feat * (g % per + 1)
        wide = [freq[...]]
        if above:
            wide.insert(0, jnp.zeros((above, rank), jnp.float32))
        if below:
            wide.append(jnp.zeros((below, rank), jnp.float32))
        basis = amp * cosine(mm(block, jnp.concatenate(wide, axis=0)) + phase[...])
        capacity[...] += mm(basis, basis / levels[:, first + g : first + g + 1], 0, 0)
    basis_own[...] = amp * cosine(mm(own[...][:, :feat], freq[...]) + phase[...])
    over = unpack(row_feat[...], n, feat)
    under = unpack(col_feat[...], n, feat)
    sq_over = jnp.sum(over * over, axis=1, keepdims=True)
    sq_under = mm(jnp.ones((8, feat), jnp.float32), under * under, 1, 1)[0:1, :]
    distance = sq_over + sq_under - 2.0 * mm(over, under, 1, 1)
    partial[...] = mm(jnp.exp(-0.5 * distance), dir_col[...])
    inverse[...] = invert(capacity[...])


def reduce_kernel(
    dims, owners, own, partial, direction, residual, basis, prior,
    sums, projected, image,
    sums_all, part, slots, blocks, send_sem, recv_sem,
):
    peers = Peers(*dims)
    me, count = peers.me, peers.count
    cols = dims[1]
    n, rhs = direction.shape
    r, c = lax.axis_index("row"), lax.axis_index("col")
    peers.greet()
    noise = own[...][:, 127:128]
    res, d = residual[...], direction[...]
    sres = res / noise
    block = pl.ds(pl.multiple_of(c * n, 8), n)
    blocks[block, :] = partial[block, :]
    peers.meet()

    def turn(k, carry):
        t = lax.rem(c + k, cols)
        peers.send(
            partial.at[pl.ds(pl.multiple_of(t * n, 8), n)],
            blocks.at[block], send_sem.at[3], recv_sem.at[3], {"row": r, "col": t},
        )
        return carry

    lax.fori_loop(1, cols, turn, 0)
    rank = projected.shape[0]
    rq = rank // owners
    proj_res = mm(basis[...], sres, 0, 0).reshape(owners, 1, rq, rhs)
    other_cols = pl.ds(0, (cols - 1) * n)
    take(blocks.at[other_cols], recv_sem.at[3])
    img = jnp.sum(blocks[...].reshape(cols, n, rhs), axis=0) + noise * d
    image[...] = img
    simg = img / noise
    mine = pl.ds(pl.multiple_of(me * 8, 8), 8)
    sums_all[mine, :] = jnp.concatenate(
        [
            jnp.sum(d * img, axis=0, keepdims=True),
            jnp.sum(res * sres, axis=0, keepdims=True),
            jnp.sum(res * simg, axis=0, keepdims=True),
            jnp.sum(img * simg, axis=0, keepdims=True),
            jnp.zeros((4, rhs), jnp.float32),
        ],
        axis=0,
    )
    proj_img = mm(basis[...], simg, 0, 0).reshape(owners, 1, rq, rhs)
    part[...] = jnp.concatenate([proj_res, proj_img], axis=1).reshape(2 * rank, rhs)
    slot = pl.ds(pl.multiple_of(me * (2 * rq), 8), 2 * rq)

    def scatter(t, dev):
        def go():
            peers.send(
                part.at[pl.ds(pl.multiple_of(t * (2 * rq), 8), 2 * rq)],
                slots.at[slot], send_sem.at[1], recv_sem.at[1], dev,
            )

        peers.send(sums_all.at[mine], sums_all.at[mine], send_sem.at[0], recv_sem.at[0], dev)
        if owners < count:
            pl.when(t < owners)(go)
        else:
            go()

    peers.each(scatter)
    other_sums = pl.ds(0, (count - 1) * 8)
    take(sums_all.at[other_sums], recv_sem.at[0])
    totals = jnp.sum(sums_all[...].reshape(count, 8, rhs), axis=0)
    sums[...] = totals
    alpha = prior[...] / totals[0:1, :]

    def owner():
        result = pl.ds(pl.multiple_of(me * rq, 8), rq)
        slots[slot, :] = part[slot, :]
        take(slots.at[pl.ds(0, (count - 1) * 2 * rq)], recv_sem.at[1])
        both = jnp.sum(slots[...].reshape(count, 2 * rq, rhs), axis=0)
        projected[result, :] = both[:rq] - alpha * both[rq:]
        if owners > 1:
            take(part.at[pl.ds(0, (owners - 1) * 2 * rq)], send_sem.at[1])
        peers.each(
            lambda t, dev: peers.send(
                projected.at[result], projected.at[result], send_sem.at[2], recv_sem.at[2], dev
            )
        )
        if owners > 1:
            take(projected.at[pl.ds(0, (owners - 1) * rq)], recv_sem.at[2])
        take(slots.at[pl.ds(0, (count - 1) * rq)], send_sem.at[2])

    def guest():
        take(projected, recv_sem.at[2])
        take(part, send_sem.at[1])

    if owners < count:
        pl.when(me < owners)(owner)
        pl.when(me >= owners)(guest)
    else:
        owner()
    take(sums_all.at[other_sums], send_sem.at[0])
    take(blocks.at[other_cols], send_sem.at[3])


def final_kernel(
    inverse, capacity, projected, sums, own, image, direction, residual, sol, basis, prior,
    new_sol, new_res, new_dir, new_prod,
):
    proj, tot = projected[...], sums[...]
    alpha = prior[...] / tot[0:1, :]
    coeffs = mm(inverse[...], proj)
    coeffs = coeffs + mm(inverse[...], proj - mm(capacity[...], coeffs))
    noise = own[...][:, 127:128]
    d = direction[...]
    nres = residual[...] - alpha * image[...]
    norm = tot[1:2, :] - 2.0 * alpha * tot[2:3, :] + alpha * alpha * tot[3:4, :]
    prod = norm - jnp.sum(proj * coeffs, axis=0, keepdims=True)
    precond = (nres - mm(basis[...], coeffs)) / noise
    new_sol[...] = sol[...] + alpha * d
    new_res[...] = nres
    new_dir[...] = precond + prod / prior[...] * d
    new_prod[...] = prod


def per_device(
    dims, points, source_ids, source_shift, noise_level, weight_in, bias_in, weight_out,
    inverse_scale, frequency, phase_shift, solution, residual, direction, prior_product,
):
    count = dims[0] * dims[1]
    n, rhs = direction.shape
    feat, rank = frequency.shape
    f32 = jnp.float32
    sds = jax.ShapeDtypeStruct
    row = lambda v: v.reshape(1, -1)
    dma = pltpu.SemaphoreType.DMA
    prior = row(prior_product)
    high = 8 * layout(n, feat)[2]
    feat_all, dir_col, own, row_feat, col_feat = pl.pallas_call(
        functools.partial(gather_kernel, dims),
        out_shape=(
            sds((count * high, 128), f32), sds((dims[0] * n, rhs), f32), sds((n, 128), f32),
            sds((dims[1] * high, 128), f32), sds((dims[0] * high, 128), f32),
        ),
        in_specs=[VMEM] * 9,
        out_specs=(VMEM,) * 5,
        scratch_shapes=[dma((2,)), dma((2,))],
        compiler_params=pltpu.CompilerParams(collective_id=0, has_side_effects=True),
        name="gather",
    )(
        points, row(source_ids), source_shift, row(noise_level), weight_in, row(bias_in),
        weight_out.T, row(inverse_scale), direction,
    )
    phase = row(phase_shift)
    square = sds((rank, rank), f32)
    inverse, capacity, partial, basis = pl.pallas_call(
        functools.partial(local_kernel, n),
        out_shape=(square, square, sds((dims[1] * n, rhs), f32), sds((n, rank), f32)),
        in_specs=[VMEM] * 7,
        out_specs=(VMEM,) * 4,
        name="local",
    )(feat_all, dir_col, row_feat, col_feat, own, frequency, phase)
    owners = min(count, rank // 8)
    sums, projected, image = pl.pallas_call(
        functools.partial(reduce_kernel, dims, owners),
        out_shape=(sds((8, rhs), f32), sds((rank, rhs), f32), sds((n, rhs), f32)),
        in_specs=[VMEM] * 6,
        out_specs=(VMEM,) * 3,
        scratch_shapes=[
            pltpu.VMEM((8 * count, rhs), f32),
            pltpu.VMEM((2 * rank, rhs), f32),
            pltpu.VMEM((count * (2 * rank // owners), rhs), f32),
            pltpu.VMEM((dims[1] * n, rhs), f32),
            dma((4,)),
            dma((4,)),
        ],
        compiler_params=pltpu.CompilerParams(collective_id=1, has_side_effects=True),
        name="reduce",
    )(own, partial, direction, residual, basis, prior)
    block = sds((n, rhs), f32)
    new_sol, new_res, new_dir, new_prod = pl.pallas_call(
        final_kernel,
        out_shape=(block, block, block, sds((1, rhs), f32)),
        in_specs=[VMEM] * 11,
        out_specs=(VMEM,) * 4,
        name="final",
    )(inverse, capacity, projected, sums, own, image, direction, residual, solution, basis, prior)
    return new_sol, new_res, new_dir, new_prod.reshape(rhs)


BF16 = jnp.bfloat16


def dot(a, b, ca=1, cb=0):
    return lax.dot_general(a, b, (((ca,), (cb,)), ((), ())), preferred_element_type=jnp.float32)


def split(x):
    high = x.astype(BF16)
    rest = x - high.astype(jnp.float32)
    mid = rest.astype(BF16)
    low = (rest - mid.astype(jnp.float32)).astype(BF16)
    return high, mid, low


def rows_of(x):
    parts = [p.astype(jnp.float32) for p in split(x)]
    fill = -3 * x.shape[0] % 16
    if fill:
        parts.append(jnp.zeros((fill, x.shape[1]), jnp.float32))
    return jnp.concatenate(parts, axis=0).astype(BF16)


def fold(acc, q):
    return acc[0:q] + acc[q : 2 * q] + acc[2 * q : 3 * q]


def iota(shape, dim):
    return lax.broadcasted_iota(jnp.int32, shape, dim)


def pivot_inverse(at):
    a00, a01, a11 = at(0, 0), at(0, 1), at(1, 1)
    b00, b01, b10, b11 = at(0, 2), at(0, 3), at(1, 2), at(1, 3)
    d00, d01, d11 = at(2, 2), at(2, 3), at(3, 3)
    inv = 1.0 / (a00 * a11 - a01 * a01)
    e00, e01, e11 = a11 * inv, -a01 * inv, a00 * inv
    f00, f01 = e00 * b00 + e01 * b10, e00 * b01 + e01 * b11
    f10, f11 = e01 * b00 + e11 * b10, e01 * b01 + e11 * b11
    s00 = d00 - (b00 * f00 + b10 * f10)
    s01 = d01 - (b00 * f01 + b10 * f11)
    s11 = d11 - (b01 * f01 + b11 * f11)
    inv = 1.0 / (s00 * s11 - s01 * s01)
    t00, t01, t11 = s11 * inv, -s01 * inv, s00 * inv
    g00, g01 = f00 * t00 + f01 * t01, f00 * t01 + f01 * t11
    g10, g11 = f10 * t00 + f11 * t01, f10 * t01 + f11 * t11
    p00 = e00 + g00 * f00 + g01 * f01
    p01 = e01 + g00 * f10 + g01 * f11
    p11 = e11 + g10 * f10 + g11 * f11
    return (
        (p00, p01, -g00, -g01),
        (p01, p11, -g10, -g11),
        (-g00, -g10, t00, t01),
        (-g01, -g11, t01, t11),
    )


def column(m, at):
    lane = lax.broadcasted_iota(jnp.int32, m.shape, 1)
    return jnp.broadcast_to(jnp.sum(jnp.where(lane == at, m, 0.0), axis=1, keepdims=True), m.shape)


def sweep(rows, first):
    size, wide = rows.shape
    groups, tiles = size // 8, wide // 128
    full = (8, 128)
    m = [[rows[8 * g : 8 * g + 8, t * 128 : (t + 1) * 128] for t in range(tiles)] for g in range(groups)]
    lane = lax.broadcasted_iota(jnp.int32, full, 1)
    sub = lax.broadcasted_iota(jnp.int32, full, 0)

    def line(x, i):
        return jnp.broadcast_to(x[i : i + 1, :], full)

    def columns(row, k):
        home, at0 = divmod(first + k, 128)
        return [column(row[home], at0 + j) for j in range(4)]

    near = columns(m[0], 0)
    for k in range(0, size, 4):
        group, off = divmod(k, 8)
        home, at0 = divmod(first + k, 128)
        cols = [columns(m[g], k) for g in range(groups)]
        pivots = pivot_inverse(lambda i, j: line(near[j], off + i))
        if k + 4 < size:
            after = (k + 4) // 8
            ahead = columns(m[after], k + 4)
            other = ahead if after == group else columns(m[group], k + 4)
            past = [[line(other[j], off + l) for l in range(4)] for j in range(4)]
            c = cols[after]
            gain = [
                (c[0] * pivots[0][l] + c[1] * pivots[1][l]) + (c[2] * pivots[2][l] + c[3] * pivots[3][l])
                for l in range(4)
            ]
            near = [
                ahead[j]
                - ((gain[0] * past[j][0] + gain[1] * past[j][1]) + (gain[2] * past[j][2] + gain[3] * past[j][3]))
                for j in range(4)
            ]
        inside = (lane >= at0) & (lane < at0 + 4)
        out = [[None] * tiles for _ in range(groups)]
        for t in range(tiles):
            own = [line(m[group][t], off + l) for l in range(4)]
            if t == home:
                own = [
                    jnp.where(lane == at0 + l, 1.0, jnp.where(inside, 0.0, own[l])) for l in range(4)
                ]
            scaled = [(p[0] * own[0] + p[1] * own[1]) + (p[2] * own[2] + p[3] * own[3]) for p in pivots]
            for g in range(groups):
                base = jnp.where(inside, 0.0, m[g][t]) if t == home else m[g][t]
                c = cols[g]
                x = base - (
                    (c[0] * scaled[0] + c[1] * scaled[1]) + (c[2] * scaled[2] + c[3] * scaled[3])
                )
                if g == group:
                    for l in range(4):
                        x = jnp.where(sub == off + l, scaled[l], x)
                out[g][t] = x
        m = out
    return jnp.concatenate([jnp.concatenate(r, axis=1) for r in m], axis=0)


def exact(a, b):
    ah, am, al = split(a)
    bh, bm, bl = split(b)
    return dot(ah, bh) + (dot(ah, bm) + dot(am, bh)) + (dot(am, bm) + dot(ah, bl) + dot(al, bh))


def invert_panels(a):
    size = a.shape[0]
    step = min(128, size)
    lane = iota((1, size), 1)
    for k in range(0, size, step):
        rows = sweep(a[k : k + step], k)
        pieces = [(k, rows)]
        for lo, hi in ((0, k), (k + step, size)):
            if hi > lo:
                part = a[lo:hi]
                base = jnp.where((lane >= k) & (lane < k + step), 0.0, part)
                pieces.append((lo, base - exact(part[:, k : k + step], rows)))
        pieces.sort(key=lambda v: v[0])
        a = jnp.concatenate([p for _, p in pieces], axis=0) if len(pieces) > 1 else rows
    return a


class Plan:
    def __init__(self, dims, n, rhs, feat):
        self.count = dims[0] * dims[1]
        self.pairs = self.count // 2
        self.n, self.rhs, self.feat = n, rhs, feat
        self.q = rhs // self.pairs
        self.per = 128 // n
        self.windows = -(-self.count // self.per)
        self.wide = 128 * self.windows
        self.groups = n // 8
        self.pieces = 128 // feat - 1
        self.tiles = -(-self.groups // self.pieces)
        self.even = dims[0] % 2 == 0

    def fits(self):
        return (
            self.even
            and self.rhs == 128
            and self.q == 8
            and 2 * self.n + 1 <= 128
            and self.per * self.n < 128
            and self.n % 8 == 0
            and self.groups <= 8
            and self.feat % 16 == 0
            and self.feat <= 32
            and self.wide <= 2048
        )


def cosine_turns(u):
    r = u - jnp.round(u)
    z = r * r
    p = SIN[-1]
    for c in SIN[-2::-1]:
        p = p * z + c
    s = p * r
    return 1.0 - 2.0 * (s * s)


SIN = tuple((-1.0) ** i * math.pi ** (2 * i + 1) / math.factorial(2 * i + 1) for i in range(7))


def pack_tiles(plan, scaled, noise):
    feat = plan.feat
    lane = iota((8, feat), 1)
    levels = jnp.zeros((8, feat), jnp.float32)
    for g in range(plan.groups):
        levels = jnp.where(lane == g, noise[8 * g : 8 * g + 8, :feat], levels)
    tiles = []
    for t in range(plan.tiles):
        row = []
        for j in range(plan.pieces):
            g = t * plan.pieces + j
            row.append(
                scaled[8 * g : 8 * g + 8] if g < plan.groups else jnp.zeros((8, feat), jnp.float32)
            )
        tiles.append(jnp.concatenate(row + [levels], axis=1))
    return tiles


def unpack_tiles(plan, feat_all):
    n, feat, per = plan.n, plan.feat, plan.per
    group = lax.rem(iota((8, 128), 1), n) // 8
    place = lax.rem(group, plan.pieces)[0:1]
    zero = jnp.zeros((8, 128), jnp.float32)
    features, levels = [], []
    for w in range(plan.windows):
        rows = []
        for k in range(per):
            s = w * per + k
            for g in range(plan.groups):
                rows.append(feat_all[s // plan.pairs, s % plan.pairs, g // plan.pieces] if s < plan.count else zero)
        rows += [zero] * (16 - len(rows))
        turned = jnp.concatenate(rows, axis=0).T
        out = turned[(plan.pieces - 1) * feat : plan.pieces * feat]
        for j in range(plan.pieces - 1):
            out = jnp.where(place == j, turned[j * feat : (j + 1) * feat], out)
        features.append(out)
        base = plan.pieces * feat
        level = jnp.where(iota((8, 128), 0) == group, turned[base : base + 8], 0.0)
        levels.append(jnp.sum(level, axis=0, keepdims=True))
    return jnp.concatenate(features, axis=1), jnp.concatenate(levels, axis=1)


def live_lanes(plan):
    lane = iota((1, plan.wide), 1)
    inside = lax.rem(lane, 128)
    source = (lane // 128) * plan.per + inside // plan.n
    return (inside < plan.per * plan.n) & (source < plan.count)


def between(lane, start, n):
    first = start % 128
    last = first + n
    if last <= 128:
        return (lane >= first) & (lane < last)
    return (lane >= first) | (lane < last - 128)


def main_kernel(
    dims, points, ids, shift, level, w_in, b_in, w_out, inv_scale, freq, phase,
    residual, direction, prior,
    res_all, dir_all,
    feat_all, turned, slabs, right, left, capacity, inverse, basis, passed, stage, send_sem, recv_sem, own_sem,
):
    peers = Peers(*dims)
    rows, cols = dims
    n, rhs = direction.shape
    feat, rank = freq.shape
    plan = Plan(dims, n, rhs, feat)
    count, pairs, q, per = plan.count, plan.pairs, plan.q, plan.per
    wide, windows = plan.wide, plan.windows
    r, c = lax.axis_index("row"), lax.axis_index("col")
    half = lax.rem(r, 2)
    pair = (r // 2) * cols + c
    me = half * pairs + pair
    f32 = jnp.float32

    def device(h, p):
        return {"row": 2 * (p // cols) + h, "col": lax.rem(p, cols)}

    sibling = {"row": 2 * (r // 2) + (1 - half), "col": c}

    def loop(first, body):
        def step(i, carry):
            body(lax.rem(2 * pairs + pair - i, pairs))
            return carry

        lax.fori_loop(first, pairs, step, 0)

    peers.greet()
    scaled, noise = features(
        points[...], ids[...], shift[...], level[...], w_in[...], b_in[...], w_out[...], inv_scale[...]
    )
    for t, tile in enumerate(pack_tiles(plan, scaled, noise)):
        feat_all[half, pair, t] = tile
    peers.meet()
    mine = feat_all.at[half, pair]
    loop(1, lambda p: peers.send(mine, mine, send_sem.at[0], recv_sem.at[0], device(half, p)))
    stacked = jnp.concatenate(
        [direction[...], residual[...], prior[...], jnp.zeros((127 - 2 * n, rhs), f32)], axis=0
    )
    spun = pltpu.roll(stacked.T, n * lax.rem(me, per), 1)
    for p in range(pairs):
        turned[p] = spun[p * q : (p + 1) * q]

    def give(p):
        peers.send(turned.at[p], slabs.at[me], send_sem.at[2], recv_sem.at[2], device(0, p))

    turn = 1.0 / (2.0 * math.pi)
    both = jnp.concatenate([freq[...], phase[...], jnp.zeros((127 - feat, rank), f32)], axis=0) * turn
    fp = both.T
    fh, fm, fl = [p.astype(f32) for p in split(fp)]
    fills = 256 - 6 * feat - 3
    spectral = jnp.concatenate(
        [fh[:, :feat], fh[:, :feat], fh[:, :feat], fm[:, :feat], fm[:, :feat], fl[:, :feat]]
        + [p[:, feat : feat + 1] for p in (fh, fm, fl)]
        + [jnp.zeros((rank, fills), f32)],
        axis=1,
    ).astype(BF16)
    lane = iota((1, 128), 1)
    live = live_lanes(plan)

    take(feat_all.at[0, pl.ds(0, pairs - 1)], recv_sem.at[0])
    peers.send(feat_all.at[half], feat_all.at[half], send_sem.at[1], recv_sem.at[1], sibling)
    loop(1, give)

    @pl.when(half == 1)
    def _():
        give(pair)

    @pl.when(half == 0)
    def _():
        slabs[me] = turned[pair]

    take(feat_all.at[0], recv_sem.at[1])
    ft, levels = unpack_tiles(plan, feat_all)
    levels = jnp.where(live, levels, 1.0)
    rsn = jnp.where(live, lax.rsqrt(levels), 0.0)
    h, m, l = split(ft)
    ft2 = ft * math.log2(math.e)
    sq = -0.5 * jnp.sum(ft2 * ft, axis=0, keepdims=True)
    sqs = [p.astype(f32) for p in split(sq)]
    ones = jnp.ones((3, wide), f32)
    rest = jnp.zeros((256 - 6 * feat - 6, wide), f32)
    right[...] = jnp.concatenate(
        [h, m, l, h, m, h, jnp.concatenate([ones] + sqs + [rest], axis=0).astype(BF16)], axis=0
    )
    amp = math.sqrt(2.0 / rank)
    u = dot(spectral, right[...])
    ch, cm, cl = split(cosine_turns(u) * (amp * rsn))
    basis[0] = ch
    basis[1] = cm
    basis[2] = cl
    tail = lane >= per * n

    @pl.when(half == 0)
    def _():
        h2, m2, l2 = split(ft2)
        low = jnp.concatenate(
            [h2, h2, h2, m2, m2, l2, jnp.concatenate(sqs + [ones, rest], axis=0).astype(BF16)], axis=0
        )
        left[...] = low.T
        take(slabs.at[pl.ds(0, count - 1)], recv_sem.at[2])
        zero = jnp.zeros((q, 128), f32)
        dirs, ress = [], []
        for w in range(windows):
            own = [slabs[w * per + k] if w * per + k < count else zero for k in range(per)]
            d, x = zero, zero
            for k in range(per):
                d = jnp.where(between(lane, k * n, n), own[k], d)
                x = jnp.where(between(lane, (k + 1) * n, n), own[k], x)
            dirs.append(d)
            ress.append(pltpu.roll(x, 128 - n, 1))
        d = jnp.concatenate(dirs, axis=1)
        res = jnp.concatenate(ress, axis=1)
        spin = pltpu.roll(slabs[me], lax.rem(128 - n * lax.rem(me, per), 128), 1)
        own_prior = spin[:, 2 * n : 2 * n + 1]
        d3 = rows_of(d)
        acc = jnp.zeros((d3.shape[0], wide), f32)
        for w in range(windows):
            k = jnp.exp2(dot(left[w * 128 : (w + 1) * 128, :], right[...]))
            kh = k.astype(BF16)
            kl = (k - kh.astype(f32)).astype(BF16)
            part = d3[:, w * 128 : (w + 1) * 128]
            acc = acc + (dot(part, kh) + dot(part, kl))
        img = fold(acc, q) + levels * d
        alpha = own_prior / jnp.sum(d * img, axis=1, keepdims=True)
        nres = res - alpha * img
        y = nres * rsn
        y3 = rows_of(y)
        proj = fold(
            dot(y3, basis[0], 1, 1) + dot(y3, basis[1], 1, 1) + dot(y3, basis[2], 1, 1), q
        )
        for w in range(windows):
            at = slice(w * 128, (w + 1) * 128)
            stage[w] = jnp.where(tail, alpha, nres[:, at])
            passed[w] = d[:, at]
            passed[windows + w] = y[:, at]
        for w in range(rank // 128):
            passed[2 * windows + w] = proj[:, w * 128 : (w + 1) * 128]
        passed[2 * windows + rank // 128] = jnp.broadcast_to(own_prior, (q, 128))
        peers.send(passed, passed, send_sem.at[3], recv_sem.at[3], sibling)
        keep = pltpu.make_async_copy(stage.at[me // per], res_all.at[pair], own_sem.at[0])
        keep.start()

        def give_rest(h, p):
            s = h * pairs + p
            peers.send(stage.at[s // per], res_all.at[pair], send_sem.at[4], recv_sem.at[4], device(h, p))

        loop(1, lambda p: give_rest(0, p))
        loop(0, lambda p: give_rest(1, p))
        keep.wait()

    @pl.when(half == 1)
    def _():
        diag = iota((rank, rank), 0) == iota((rank, rank), 1)
        cross = dot(ch, cm, 1, 1) + dot(ch, cl, 1, 1)
        capacity[...] = (
            jnp.where(diag, 1.0, 0.0) + (dot(ch, ch, 1, 1) + dot(cm, cm, 1, 1)) + (cross + cross.T)
        )
        inverse[...] = invert_panels(capacity[...])
        take(passed, recv_sem.at[3])
        proj = jnp.concatenate([passed[2 * windows + w] for w in range(rank // 128)], axis=1)
        p3 = rows_of(proj)
        ih, im, il = split(inverse[...])
        c3 = rows_of(fold(dot(p3, ih) + dot(p3, im) + dot(p3, il), q))
        back = fold(dot(c3, basis[0]) + dot(c3, basis[1]) + dot(c3, basis[2]), q)
        d = jnp.concatenate([passed[w] for w in range(windows)], axis=1)
        y = jnp.concatenate([passed[windows + w] for w in range(windows)], axis=1)
        own_prior = passed[2 * windows + rank // 128][:, 0:1]
        gap = y - back
        prod = jnp.sum(y * gap, axis=1, keepdims=True)
        ndir = gap * rsn + prod / own_prior * d
        for w in range(windows):
            stage[w] = jnp.where(tail, prod, ndir[:, w * 128 : (w + 1) * 128])
        keep = pltpu.make_async_copy(stage.at[me // per], dir_all.at[pair], own_sem.at[0])
        keep.start()

        def give_dir(h, p):
            s = h * pairs + p
            peers.send(stage.at[s // per], dir_all.at[pair], send_sem.at[4], recv_sem.at[5], device(h, p))

        loop(1, lambda p: give_dir(1, p))
        loop(0, lambda p: give_dir(0, p))
        keep.wait()

    @pl.when(half == 0)
    def _():
        take(slabs.at[pl.ds(0, pairs - 1)], send_sem.at[2])
        take(passed, send_sem.at[3])
        take(res_all.at[pl.ds(0, pairs - 1)], recv_sem.at[4])
        take(dir_all, recv_sem.at[5])

    @pl.when(half == 1)
    def _():
        take(slabs.at[pl.ds(0, pairs)], send_sem.at[2])
        take(res_all, recv_sem.at[4])
        take(dir_all.at[pl.ds(0, pairs - 1)], recv_sem.at[5])

    take(feat_all.at[0, pl.ds(0, pairs - 1)], send_sem.at[0])
    take(feat_all.at[0], send_sem.at[1])
    take(slabs.at[pl.ds(0, count - 1)], send_sem.at[4])


def finish_kernel(dims, res, dirs, direction, sol, new_sol, new_res, new_dir, new_prod, spare):
    r, c = lax.axis_index("row"), lax.axis_index("col")
    me = lax.rem(r, 2) * (dims[0] * dims[1] // 2) + (r // 2) * dims[1] + c
    n = direction.shape[0]
    own = pl.ds(pl.multiple_of(n * lax.rem(me, 128 // n), 8), n)
    x = res[...].T
    spare[...] = x
    new_res[...] = spare[own, :]
    new_sol[...] = sol[...] + x[127:128] * direction[...]
    z = dirs[...].T
    spare[...] = z
    new_dir[...] = spare[own, :]
    new_prod[...] = z[127:128]


def per_device_columns(
    dims, points, source_ids, source_shift, noise_level, weight_in, bias_in, weight_out,
    inverse_scale, frequency, phase_shift, solution, residual, direction, prior_product,
):
    n, rhs = direction.shape
    feat, rank = frequency.shape
    plan = Plan(dims, n, rhs, feat)
    count, pairs, q, wide, windows = plan.count, plan.pairs, plan.q, plan.wide, plan.windows
    f32 = jnp.float32
    sds = jax.ShapeDtypeStruct
    row = lambda v: v.reshape(1, -1)
    dma = pltpu.SemaphoreType.DMA
    res, dirs = pl.pallas_call(
        functools.partial(main_kernel, dims),
        out_shape=(sds((pairs, q, 128), f32), sds((pairs, q, 128), f32)),
        in_specs=[VMEM] * 13,
        out_specs=(pl.BlockSpec(memory_space=pltpu.HBM),) * 2,
        scratch_shapes=[
            pltpu.VMEM((2, pairs, plan.tiles, 8, 128), f32),
            pltpu.VMEM((pairs, q, 128), f32),
            pltpu.VMEM((count, q, 128), f32),
            pltpu.VMEM((256, wide), BF16),
            pltpu.VMEM((wide, 256), BF16),
            pltpu.VMEM((rank, rank), f32),
            pltpu.VMEM((rank, rank), f32),
            pltpu.VMEM((3, rank, wide), BF16),
            pltpu.VMEM((2 * windows + rank // 128 + 1, q, 128), f32),
            pltpu.VMEM((windows, q, 128), f32),
            dma((6,)),
            dma((6,)),
            dma((1,)),
        ],
        compiler_params=pltpu.CompilerParams(collective_id=0, has_side_effects=True),
        name="columns",
    )(
        points, row(source_ids), source_shift, row(noise_level), weight_in, row(bias_in),
        weight_out.T, row(inverse_scale), frequency, row(phase_shift), residual, direction,
        row(prior_product),
    )
    block = sds((n, rhs), f32)
    new_sol, new_res, new_dir, new_prod = pl.pallas_call(
        functools.partial(finish_kernel, dims),
        out_shape=(block, block, block, sds((1, rhs), f32)),
        in_specs=[VMEM] * 4,
        out_specs=(VMEM,) * 4,
        scratch_shapes=[pltpu.VMEM((128, rhs), f32)],
        name="finish",
    )(res.reshape(rhs, 128), dirs.reshape(rhs, 128), direction, solution)
    return new_sol, new_res, new_dir, new_prod.reshape(rhs)


def dispatch(dims, *args):
    n, rhs = args[12].shape
    feat = args[8].shape[0]
    if Plan(dims, n, rhs, feat).fits():
        return per_device_columns(dims, *args)
    return per_device(dims, *args)


def solution(mesh):
    dims = (mesh.shape["row"], mesh.shape["col"])
    rows = P(("row", "col"), None)
    in_specs = (
        rows, P(("row", "col")), P(), P(), P(), P(), P(), P(), P(), P(), rows, rows, rows, P(),
    )
    return jax.shard_map(
        functools.partial(dispatch, dims),
        mesh=mesh,
        in_specs=in_specs,
        out_specs=(rows, rows, rows, P()),
        check_vma=False,
    )
```
